32 devices in a mesh: vocab: 4 (over y, x), dp: 8 (over z, core).
Axes of the slice: x: 2, y: 2, z: 4, core: 2. Of those that a mesh axis runs over, the one named last changes fastest.
Arguments:
- grads: bfloat16 [4096, 4096], P(('vocab', 'dp')), may hold values from -6 to 6
- token_ids: int32 [4096], P(('vocab', 'dp')), may hold values from 0 to 32063, as said below
Outputs:
- grad_table: float32 [32064, 4096], P('vocab', 'dp')
- row_share: float32 [32064], P('vocab')
The draws below stay inside these ranges and needn't reach their ends.
Inputs may be any that keep to these rules, and one draw needn't show every extreme that they name: `token_ids`: within the 128 ids of one device (aligned blocks in order) the ids never fall; at most 32 of them lie in the rows k * 8016 to (k + 1) * 8016 - 1 of any one k, and in every block some k has exactly 32.
All inputs are finite; a program needn't handle non-finite values.
Results may differ from the reference program's by a relative error of at most 0.0003.
Values may be sent and summed in bfloat16 or wider, within the bound.
No kernel may reach another device: no remote copies, remote signals or barrier semaphores. Data moves between devices by JAX's collectives and lax.ppermute only.
A program may use at most 64 MiB of HBM per device.

```python
import jax
import jax.numpy as jnp
from jax import lax

D = 4096
VOCAB_DEV = 8016
TOK_DEV = 128
CAP = 32
VOCAB = 32064
TOKENS = 4096
N_VOCAB = 4


def one_block(key):
    owners = VOCAB // VOCAB_DEV
    base = TOK_DEV // owners
    order = jax.random.permutation(jax.random.fold_in(key, 1), owners)
    top = order[0]
    lowest = order[1]
    counts = jnp.full((owners,), base, jnp.int32)
    counts = counts.at[top].set(CAP).at[lowest].set(2 * base - CAP)
    for turn in range(6):
        sub_key = jax.random.fold_in(key, 10 + turn)
        paired = jax.random.permutation(sub_key, owners)
        first = paired[0]
        second = paired[1]
        keep = jnp.where(second == top, CAP, 0)
        limit = jnp.minimum(CAP - counts[first], counts[second] - keep)
        moved = jax.random.randint(jax.random.fold_in(sub_key, 5), (), 0, limit + 1)
        counts = counts.at[first].add(moved).at[second].add(-moved)
    ends = jnp.cumsum(counts)
    places = jnp.arange(TOK_DEV, dtype=jnp.int32)
    owner_of = jnp.sum((places[:, None] >= ends[None, :]).astype(jnp.int32), axis=1)
    inner = jax.random.randint(jax.random.fold_in(key, 3), (TOK_DEV,), 0, VOCAB_DEV)
    return jnp.sort(owner_of * VOCAB_DEV + inner)


def draw_token_ids(key, part):
    blocks = TOKENS // TOK_DEV
    keys = jax.random.split(jax.random.fold_in(key, 77), blocks)
    return jax.vmap(one_block)(keys).reshape(-1).astype(jnp.int32)


def level_of(own_key, extent, shards, smallest, high):
    def one(axis_at, blocks):
        heights = jax.random.uniform(jax.random.fold_in(jax.random.fold_in(own_key, 6), axis_at), (blocks,), jnp.float32, smallest / len(shards), high / len(shards))
        return jnp.repeat(jnp.exp(heights), extent[axis_at] // blocks).reshape((-1,) + (1,) * (len(extent) - axis_at - 1))

    level = one(*shards[0])
    for cut in shards[1:]:
        level = level * one(*cut)
    return level


def scatter_about(own_key, extent, width, reach, cuts=(), kind=jnp.bfloat16):
    factor_of = level_of(own_key, extent, cuts, -0.22, 0.18) if cuts else 1.0
    drawn = jax.random.normal(own_key, extent, jnp.float32) * width * factor_of
    return jnp.minimum(jnp.maximum(drawn, -reach), reach).astype(kind)


def setup_inputs(seed: int = 0) -> dict:
    splits = jax.random.split(jax.random.key(seed), 3)
    return {
        "grads": scatter_about(splits[0], (TOKENS, D), 1.0, 6.0, ((0, 32),)),
        "token_ids": draw_token_ids(jax.random.fold_in(splits[2], 71), 0),
    }


def reference(grads, token_ids):
    vocab_total = VOCAB_DEV * N_VOCAB
    grad_blocks = grads.reshape(-1, TOK_DEV, D)
    id_blocks = token_ids.reshape(-1, TOK_DEV)

    def accumulate(carry, item):
        table, counts = carry
        block, ids = item
        table = table + jax.ops.segment_sum(block.astype(jnp.float32), ids, num_segments=vocab_total)
        counts = counts + jax.ops.segment_sum(jnp.ones((TOK_DEV,), jnp.float32), ids, num_segments=vocab_total)
        return (table, counts), None

    start = (jnp.zeros((vocab_total, D), jnp.float32), jnp.zeros((vocab_total,), jnp.float32))
    (table, counts), _ = lax.scan(accumulate, start, (grad_blocks, id_blocks))
    row_share = counts * (vocab_total / TOKENS)
    return table, row_share
```

```python
import jax
import jax.numpy as jnp
from jax import lax
from jax.sharding import PartitionSpec as P

VOCAB_DEV = 8016
TOK_DEV = 128
CAP = 32
AXES = ("vocab", "dp")


def bucket(ids, data, n_vocab):
    owner_start = jnp.arange(n_vocab, dtype=jnp.int32) * VOCAB_DEV
    length = ids.shape[0]
    if n_vocab * CAP == length:
        return data, ids.reshape(n_vocab, CAP) - owner_start[:, None]
    starts = jnp.sum((ids[None, :] < owner_start[:, None]).astype(jnp.int32), axis=1)
    finish = jnp.concatenate([starts[1:], jnp.full((1,), length, jnp.int32)])
    slot = jnp.arange(CAP, dtype=jnp.int32)
    places = starts[:, None] + slot[None, :]
    valid = places < finish[:, None]
    columns = jnp.arange(length, dtype=jnp.int32)
    select = (places[:, :, None] == columns) & valid[:, :, None]
    rows = jnp.einsum(
        "vcl,ld->vcd", select.astype(data.dtype), data, preferred_element_type=jnp.float32
    ).astype(data.dtype)
    picked = jnp.sum(jnp.where(select, ids, 0), axis=2)
    slot_ids = jnp.where(valid, picked - owner_start[:, None], -1)
    return rows.reshape(n_vocab * CAP, data.shape[1]), slot_ids


def local(grads, token_ids):
    n_vocab = lax.axis_size("vocab")
    n_data = lax.axis_size("dp")
    width = grads.shape[1] // n_data
    rows, slot_ids = bucket(token_ids, grads, n_vocab)
    rows = rows.reshape(n_vocab, CAP, n_data, width).transpose(0, 2, 1, 3)
    rows = rows.reshape(n_vocab * n_data, CAP, width)
    slot_ids = jnp.broadcast_to(slot_ids[:, None, :], (n_vocab, n_data, CAP)).reshape(n_vocab * n_data, CAP)
    mine = lax.all_to_all(rows, AXES, split_axis=0, concat_axis=0, tiled=True)
    mine_ids = lax.all_to_all(slot_ids, AXES, split_axis=0, concat_axis=0, tiled=True)
    mine = mine.reshape(-1, width)
    mine_ids = mine_ids.reshape(-1)
    table_rows = jnp.arange(VOCAB_DEV, dtype=jnp.int32)
    onehot = table_rows[:, None] == mine_ids[None, :]
    table = lax.dot_general(
        onehot.astype(mine.dtype), mine, (((1,), (0,)), ((), ())), preferred_element_type=jnp.float32
    )
    counts = jnp.sum(onehot.astype(jnp.float32), axis=1)
    return table, counts * (VOCAB_DEV / (TOK_DEV * n_data))


def solution(mesh):
    in_specs = (P(AXES, None), P(AXES))
    out_specs = (P("vocab", "dp"), P("vocab"))
    return jax.shard_map(local, mesh=mesh, in_specs=in_specs, out_specs=out_specs, check_vma=False)
```

```python
import functools

import jax
import jax.numpy as jnp
from jax import lax
from jax.experimental import pallas as pl
from jax.experimental.pallas import tpu as pltpu
from jax.sharding import PartitionSpec as P

VOCAB_DEV = 8016
TOK_DEV = 128
CAP = 32
AXES = ("vocab", "dp")
LANES = 128
GROUP = LANES // CAP
ID_ROWS = 8
BLOCK = 512
PAIR = 2
BLOCKS = -(-VOCAB_DEV // (BLOCK * PAIR)) * PAIR
WINDOW = 256


def bucket(ids, data, n_vocab):
    length = ids.shape[0]
    if n_vocab * CAP == length:
        return data, ids.reshape(1, length)
    owner_start = jnp.arange(n_vocab, dtype=jnp.int32) * VOCAB_DEV
    starts = jnp.sum((ids[None, :] < owner_start[:, None]).astype(jnp.int32), axis=1)
    finish = jnp.concatenate([starts[1:], jnp.full((1,), length, jnp.int32)])
    slot = jnp.arange(CAP, dtype=jnp.int32)
    places = starts[:, None] + slot[None, :]
    valid = places < finish[:, None]
    columns = jnp.arange(length, dtype=jnp.int32)
    select = (places[:, :, None] == columns) & valid[:, :, None]
    rows = jnp.einsum(
        "vcl,ld->vcd", select.astype(data.dtype), data, preferred_element_type=jnp.float32
    ).astype(data.dtype)
    picked = jnp.sum(jnp.where(select, ids, 0), axis=2)
    slot_ids = jnp.where(valid, picked, -1)
    return rows.reshape(n_vocab * CAP, data.shape[1]), slot_ids.reshape(1, n_vocab * CAP)


def pack_kernel(n_vocab, n_data, rows_hbm, ids_ref, out_hbm, rows, out, in_sem, out_sem):
    tiles = rows.shape[1] // (n_data * LANES)
    loads = []
    for v in range(n_vocab):
        strip = pl.ds(v * CAP, CAP)
        loads.append(pltpu.make_async_copy(rows_hbm.at[strip], rows.at[strip], in_sem.at[v]))
        loads[-1].start()
    source = lax.axis_index("vocab") * n_data + lax.axis_index("dp")
    lane = lax.broadcasted_iota(jnp.int32, (ID_ROWS, LANES), 1)
    sub = lax.broadcasted_iota(jnp.int32, (ID_ROWS, LANES), 0)
    row = lax.rem(lax.div(source, GROUP), ID_ROWS // 2)
    here = lax.div(lane, CAP) == lax.rem(source, GROUP)
    stores = []
    for v in range(n_vocab):
        ids = ids_ref[:, v * CAP : (v + 1) * CAP]
        ids = jnp.where(ids < 0, -1, ids - v * VOCAB_DEV)
        ids = jnp.concatenate([ids] * GROUP, axis=1)
        high = lax.shift_right_arithmetic(ids, 7).astype(jnp.float32)
        low = jnp.bitwise_and(ids, 127).astype(jnp.float32)
        coded = jnp.where(here & (sub == row), high, 0.0) + jnp.where(here & (sub == row + ID_ROWS // 2), low, 0.0)
        coded = coded.astype(out.dtype)
        loads[v].wait()
        for d in range(n_data):
            for j in range(tiles):
                column = (d * tiles + j) * LANES
                out[v * n_data + d, j * CAP : (j + 1) * CAP, :] = rows[
                    v * CAP : (v + 1) * CAP, column : column + LANES
                ]
            out[v * n_data + d, tiles * CAP : tiles * CAP + ID_ROWS, :] = coded
        strip = pl.ds(v * n_data, n_data)
        stores.append(pltpu.make_async_copy(out.at[strip], out_hbm.at[strip], out_sem.at[v]))
        stores[-1].start()
    for store in stores:
        store.wait()


def pack(rows, ids, n_vocab, n_data):
    width = rows.shape[1] // n_data
    length = width // LANES * CAP + ID_ROWS
    shape = (n_vocab * n_data, length, LANES)
    return pl.pallas_call(
        functools.partial(pack_kernel, n_vocab, n_data),
        out_shape=jax.ShapeDtypeStruct(shape, rows.dtype),
        in_specs=[pl.BlockSpec(memory_space=pl.ANY), pl.BlockSpec(memory_space=pltpu.VMEM)],
        out_specs=pl.BlockSpec(memory_space=pl.ANY),
        scratch_shapes=[
            pltpu.VMEM(rows.shape, rows.dtype),
            pltpu.VMEM(shape, rows.dtype),
            pltpu.SemaphoreType.DMA((n_vocab,)),
            pltpu.SemaphoreType.DMA((n_vocab,)),
        ],
        name="pack",
    )(rows, ids)


def table_kernel(
    scale, got, table_hbm, share_ref, x, ids_s, key_s, column_s, rank_s, sorted_ids, sorted_columns, sorted_x, table, starts, sem
):
    sources, length, _ = got.shape
    total = sources * CAP
    chunks = total // LANES
    tiles = (length - ID_ROWS) // CAP
    half = ID_ROWS // 2
    per = half * GROUP
    for g in range(sources // per):
        coded = got[g * per, tiles * CAP :, :].astype(jnp.float32)
        for s in range(g * per + 1, (g + 1) * per):
            coded = coded + got[s, tiles * CAP :, :].astype(jnp.float32)
        ids_s[g * half : (g + 1) * half, :] = (coded[:half] * 128.0 + coded[half:]).astype(jnp.int32)
    ids = ids_s[...]
    ids = jnp.where(ids < 0, BLOCKS * BLOCK, ids)
    token = lax.broadcasted_iota(jnp.int32, (chunks, LANES), 0) * LANES + lax.broadcasted_iota(
        jnp.int32, (chunks, LANES), 1
    )
    key = ids * total + token
    key_s[...] = key
    turned = key.T
    for q in range(chunks):
        column_s[q * LANES : (q + 1) * LANES, :] = jnp.broadcast_to(turned[:, q : q + 1], (LANES, LANES))
    for b in range(BLOCKS + 1):
        starts[b] = jnp.sum((ids < b * BLOCK).astype(jnp.int32))
    for j in range(tiles):
        x[:, j * LANES : (j + 1) * LANES] = got[:, j * CAP : (j + 1) * CAP, :].reshape(total, LANES)

    def count(q, before):
        column = column_s[pl.ds(pl.multiple_of(q * LANES, LANES), LANES), :].reshape(LANES // 8, 8, LANES)
        return tuple(
            before[p] + jnp.sum((column < key_s[p : p + 1, :].reshape(1, 1, LANES)).astype(jnp.int32), axis=0)
            for p in range(chunks)
        )

    before = lax.fori_loop(0, chunks, count, tuple(jnp.zeros((8, LANES), jnp.int32) for _ in range(chunks)))
    for p in range(chunks):
        rank_s[p : p + 1, :] = jnp.sum(before[p], axis=0, keepdims=True)

    flat = jnp.concatenate([ids[p : p + 1, :] for p in range(chunks)], axis=1)
    pick = lax.broadcasted_iota(jnp.int32, (8, total), 0)
    parts = jnp.where(pick == 0, lax.shift_right_arithmetic(flat, 7), jnp.bitwise_and(flat, 127))
    parts = parts.astype(jnp.float32).astype(x.dtype)

    def order(c, _):
        place = lax.broadcasted_iota(jnp.int32, (WINDOW, LANES), 0) + c * WINDOW
        move = jnp.concatenate(
            [jnp.where(rank_s[p : p + 1, :] == place, 1.0, 0.0).astype(x.dtype) for p in range(chunks)], axis=1
        )
        at = pl.ds(pl.multiple_of(c * WINDOW, WINDOW), WINDOW)
        sorted_x[at, :] = jnp.dot(move, x[...], preferred_element_type=jnp.float32).astype(x.dtype)
        moved = lax.dot_general(parts, move, (((1,), (1,)), ((), ())), preferred_element_type=jnp.float32)
        moved = (moved[0:1] * 128.0 + moved[1:2]).astype(jnp.int32)
        for i in range(WINDOW // LANES):
            sorted_ids[pl.ds(c * (WINDOW // LANES) + i, 1), :] = moved[:, i * LANES : (i + 1) * LANES]
        return 0

    lax.fori_loop(0, total // WINDOW, order, 0)
    sorted_ids[chunks : chunks + 8, :] = jnp.full((8, LANES), -1, jnp.int32)
    sorted_x[total : total + LANES, :] = jnp.zeros((LANES, x.shape[1]), x.dtype)
    turned = sorted_ids[...].T
    for q in range(chunks + 1):
        sorted_columns[q * LANES : (q + 1) * LANES, :] = jnp.broadcast_to(turned[:, q : q + 1], (LANES, LANES))

    def rows_of(b, k):
        place = lax.broadcasted_iota(jnp.int32, (BLOCK, LANES), 0) + b * BLOCK
        hit = jnp.concatenate(
            [
                jnp.where(sorted_ids[pl.ds(k + i, 1), :] == place, 1.0, 0.0).astype(x.dtype)
                for i in range(WINDOW // LANES)
            ],
            axis=1,
        )
        at = pl.ds(pl.multiple_of(k * LANES, LANES), WINDOW)
        return jnp.dot(hit, sorted_x[at, :], preferred_element_type=jnp.float32)

    def counts_of(b, k):
        column = sorted_columns[pl.ds(pl.multiple_of(k * LANES, LANES), WINDOW), :].reshape(WINDOW // 8, 8, LANES)
        place = lax.broadcasted_iota(jnp.int32, (1, 1, LANES), 2) + b * BLOCK
        return jnp.concatenate(
            [
                jnp.sum(jnp.sum((column == place + i * LANES).astype(jnp.float32), axis=0), axis=0, keepdims=True)
                for i in range(BLOCK // LANES)
            ],
            axis=0,
        )

    last = BLOCKS - 1
    rest = VOCAB_DEV - last * BLOCK

    def out_copy(b, n):
        at = pl.ds(pl.multiple_of(b * BLOCK, BLOCK), n)
        return pltpu.make_async_copy(table.at[at, :], table_hbm.at[at, :], sem.at[b])

    def build(step, _):
        for i in range(PAIR):
            b = step * PAIR + i
            k = jnp.minimum(lax.shift_right_logical(starts[b], 7), chunks - 1)
            table[pl.ds(pl.multiple_of(b * BLOCK, BLOCK), BLOCK), :] = rows_of(b, k)
            share_ref[pl.ds(b * (BLOCK // LANES), BLOCK // LANES), :] = counts_of(b, k) * scale
        for i in range(PAIR):
            b = step * PAIR + i
            k = jnp.minimum(lax.shift_right_logical(starts[b], 7), chunks - 1)
            more = lax.div(jnp.maximum(starts[b + 1] - k * LANES - 1, 0), WINDOW)

            def further(w, _, b=b, k=k):
                at = pl.ds(pl.multiple_of(b * BLOCK, BLOCK), BLOCK)
                table[at, :] += rows_of(b, k + w * (WINDOW // LANES))
                at = pl.ds(b * (BLOCK // LANES), BLOCK // LANES)
                share_ref[at, :] += counts_of(b, k + w * (WINDOW // LANES)) * scale
                return 0

            lax.fori_loop(1, more + 1, further, 0)

            @pl.when(b < last)
            def _(b=b):
                out_copy(b, BLOCK).start()

            @pl.when(b == last)
            def _():
                out_copy(last, rest).start()

        return 0

    lax.fori_loop(0, BLOCKS // PAIR, build, 0)
    for b in range(last):
        out_copy(b, BLOCK).wait()
    out_copy(last, rest).wait()


def make_table(got, scale):
    sources, length, _ = got.shape
    total = sources * CAP
    chunks = total // LANES
    width = (length - ID_ROWS) // CAP * LANES
    return pl.pallas_call(
        functools.partial(table_kernel, scale),
        out_shape=(
            jax.ShapeDtypeStruct((VOCAB_DEV, width), jnp.float32),
            jax.ShapeDtypeStruct((BLOCKS * BLOCK // LANES, LANES), jnp.float32),
        ),
        in_specs=[pl.BlockSpec(memory_space=pltpu.VMEM)],
        out_specs=(pl.BlockSpec(memory_space=pl.ANY), pl.BlockSpec(memory_space=pltpu.VMEM)),
        scratch_shapes=[
            pltpu.VMEM((total, width), got.dtype),
            pltpu.VMEM((chunks, LANES), jnp.int32),
            pltpu.VMEM((chunks, LANES), jnp.int32),
            pltpu.VMEM((total, LANES), jnp.int32),
            pltpu.VMEM((chunks, LANES), jnp.int32),
            pltpu.VMEM((chunks + 8, LANES), jnp.int32),
            pltpu.VMEM((total + LANES, LANES), jnp.int32),
            pltpu.VMEM((total + LANES, width), got.dtype),
            pltpu.VMEM((BLOCKS * BLOCK, width), jnp.float32),
            pltpu.SMEM((BLOCKS + 1,), jnp.int32),
            pltpu.SemaphoreType.DMA((BLOCKS,)),
        ],
        compiler_params=pltpu.CompilerParams(vmem_limit_bytes=48 * 1024 * 1024),
        name="table",
    )(got)


def local(grads, token_ids):
    n_vocab = lax.axis_size("vocab")
    n_data = lax.axis_size("dp")
    rows, ids = bucket(token_ids, grads, n_vocab)
    sent = pack(rows, ids, n_vocab, n_data)
    got = lax.all_to_all(sent, AXES, split_axis=0, concat_axis=0, tiled=True)
    table, share = make_table(got, VOCAB_DEV / (TOK_DEV * n_data))
    return table, share.reshape(-1)[:VOCAB_DEV]


def solution(mesh):
    in_specs = (P(AXES, None), P(AXES))
    out_specs = (P("vocab", "dp"), P("vocab"))
    return jax.shard_map(local, mesh=mesh, in_specs=in_specs, out_specs=out_specs, check_vma=False)
```

```python
import functools

import jax
import jax.numpy as jnp
from jax import lax
from jax.experimental import pallas as pl
from jax.experimental.pallas import tpu as pltpu
from jax.sharding import PartitionSpec as P

VOCAB_DEV = 8016
TOK_DEV = 128
CAP = 32
AXES = ("vocab", "dp")
LANES = 128
GROUP = LANES // CAP
ID_ROWS = 8
BLOCK = 512
BLOCKS = -(-VOCAB_DEV // BLOCK)
WINDOW = 256


def bucket(ids, data, n_vocab):
    length = ids.shape[0]
    if n_vocab * CAP == length:
        return data, ids.reshape(1, length)
    owner_start = jnp.arange(n_vocab, dtype=jnp.int32) * VOCAB_DEV
    starts = jnp.sum((ids[None, :] < owner_start[:, None]).astype(jnp.int32), axis=1)
    finish = jnp.concatenate([starts[1:], jnp.full((1,), length, jnp.int32)])
    slot = jnp.arange(CAP, dtype=jnp.int32)
    places = starts[:, None] + slot[None, :]
    valid = places < finish[:, None]
    columns = jnp.arange(length, dtype=jnp.int32)
    select = (places[:, :, None] == columns) & valid[:, :, None]
    rows = jnp.einsum(
        "vcl,ld->vcd", select.astype(data.dtype), data, preferred_element_type=jnp.float32
    ).astype(data.dtype)
    picked = jnp.sum(jnp.where(select, ids, 0), axis=2)
    slot_ids = jnp.where(valid, picked, -1)
    return rows.reshape(n_vocab * CAP, data.shape[1]), slot_ids.reshape(1, n_vocab * CAP)


def pack_kernel(n_vocab, n_data, rows_hbm, ids_ref, out_hbm, rows, out, in_sem, out_sem):
    tiles = rows.shape[1] // (n_data * LANES)
    loads = []
    for v in range(n_vocab):
        strip = pl.ds(v * CAP, CAP)
        loads.append(pltpu.make_async_copy(rows_hbm.at[strip], rows.at[strip], in_sem.at[v]))
        loads[-1].start()
    source = lax.axis_index("vocab") * n_data + lax.axis_index("dp")
    lane = lax.broadcasted_iota(jnp.int32, (ID_ROWS, LANES), 1)
    sub = lax.broadcasted_iota(jnp.int32, (ID_ROWS, LANES), 0)
    row = lax.rem(lax.div(source, GROUP), ID_ROWS // 2)
    here = lax.div(lane, CAP) == lax.rem(source, GROUP)
    stores = []
    for v in range(n_vocab):
        ids = ids_ref[:, v * CAP : (v + 1) * CAP]
        ids = jnp.where(ids < 0, -1, ids - v * VOCAB_DEV)
        ids = jnp.concatenate([ids] * GROUP, axis=1)
        high = lax.shift_right_arithmetic(ids, 7).astype(jnp.float32)
        low = jnp.bitwise_and(ids, 127).astype(jnp.float32)
        coded = jnp.where(here & (sub == row), high, 0.0) + jnp.where(here & (sub == row + ID_ROWS // 2), low, 0.0)
        coded = coded.astype(out.dtype)
        loads[v].wait()
        for d in range(n_data):
            for j in range(tiles):
                column = (d * tiles + j) * LANES
                out[v * n_data + d, j * CAP : (j + 1) * CAP, :] = rows[
                    v * CAP : (v + 1) * CAP, column : column + LANES
                ]
            out[v * n_data + d, tiles * CAP : tiles * CAP + ID_ROWS, :] = coded
        strip = pl.ds(v * n_data, n_data)
        stores.append(pltpu.make_async_copy(out.at[strip], out_hbm.at[strip], out_sem.at[v]))
        stores[-1].start()
    for store in stores:
        store.wait()


def pack(rows, ids, n_vocab, n_data):
    width = rows.shape[1] // n_data
    length = width // LANES * CAP + ID_ROWS
    shape = (n_vocab * n_data, length, LANES)
    return pl.pallas_call(
        functools.partial(pack_kernel, n_vocab, n_data),
        out_shape=jax.ShapeDtypeStruct(shape, rows.dtype),
        in_specs=[pl.BlockSpec(memory_space=pl.ANY), pl.BlockSpec(memory_space=pltpu.VMEM)],
        out_specs=pl.BlockSpec(memory_space=pl.ANY),
        scratch_shapes=[
            pltpu.VMEM(rows.shape, rows.dtype),
            pltpu.VMEM(shape, rows.dtype),
            pltpu.SemaphoreType.DMA((n_vocab,)),
            pltpu.SemaphoreType.DMA((n_vocab,)),
        ],
        name="pack",
    )(rows, ids)


def table_kernel(
    scale, got, table_hbm, share_hbm, x, ids_s, key_s, column_s, rank_s, sorted_ids, sorted_columns, sorted_x, table, share, starts, sem
):
    sources, length, _ = got.shape
    total = sources * CAP
    chunks = total // LANES
    tiles = (length - ID_ROWS) // CAP
    half = ID_ROWS // 2
    per = half * GROUP
    for g in range(sources // per):
        coded = got[g * per, tiles * CAP :, :].astype(jnp.float32)
        for s in range(g * per + 1, (g + 1) * per):
            coded = coded + got[s, tiles * CAP :, :].astype(jnp.float32)
        ids_s[g * half : (g + 1) * half, :] = (coded[:half] * 128.0 + coded[half:]).astype(jnp.int32)
    ids = ids_s[...]
    ids = jnp.where(ids < 0, BLOCKS * BLOCK, ids)
    token = lax.broadcasted_iota(jnp.int32, (chunks, LANES), 0) * LANES + lax.broadcasted_iota(
        jnp.int32, (chunks, LANES), 1
    )
    key = ids * total + token
    key_s[...] = key
    turned = key.T
    for q in range(chunks):
        column_s[q * LANES : (q + 1) * LANES, :] = jnp.broadcast_to(turned[:, q : q + 1], (LANES, LANES))
    for b in range(BLOCKS + 1):
        starts[b] = jnp.sum((ids < b * BLOCK).astype(jnp.int32))
    for j in range(tiles):
        x[:, j * LANES : (j + 1) * LANES] = got[:, j * CAP : (j + 1) * CAP, :].reshape(total, LANES)

    def count(q, before):
        column = column_s[pl.ds(pl.multiple_of(q * LANES, LANES), LANES), :].reshape(LANES // 8, 8, LANES)
        return tuple(
            before[p] + jnp.sum((column < key_s[p : p + 1, :].reshape(1, 1, LANES)).astype(jnp.int32), axis=0)
            for p in range(chunks)
        )

    before = lax.fori_loop(0, chunks, count, tuple(jnp.zeros((8, LANES), jnp.int32) for _ in range(chunks)))
    for p in range(chunks):
        rank_s[p : p + 1, :] = jnp.sum(before[p], axis=0, keepdims=True)

    sorted_ids[...] = jnp.full(sorted_ids.shape, -1, jnp.int32)
    sorted_columns[...] = jnp.full(sorted_columns.shape, -1, jnp.int32)
    sorted_x[...] = jnp.zeros(sorted_x.shape, x.dtype)
    flat = jnp.concatenate([ids[p : p + 1, :] for p in range(chunks)], axis=1)
    pick = lax.broadcasted_iota(jnp.int32, (8, total), 0)
    parts = jnp.where(pick == 0, lax.shift_right_arithmetic(flat, 7), jnp.bitwise_and(flat, 127))
    parts = parts.astype(jnp.float32).astype(x.dtype)

    def order(c):
        place = lax.broadcasted_iota(jnp.int32, (WINDOW, LANES), 0) + c * WINDOW
        move = jnp.concatenate(
            [jnp.where(rank_s[p : p + 1, :] == place, 1.0, 0.0).astype(x.dtype) for p in range(chunks)], axis=1
        )
        sorted_x[c * WINDOW : (c + 1) * WINDOW, :] = jnp.dot(move, x[...], preferred_element_type=jnp.float32).astype(x.dtype)
        moved = lax.dot_general(parts, move, (((1,), (1,)), ((), ())), preferred_element_type=jnp.float32)
        moved = (moved[0:1] * 128.0 + moved[1:2]).astype(jnp.int32)
        for i in range(WINDOW // LANES):
            at = c * (WINDOW // LANES) + i
            sorted_ids[at : at + 1, :] = moved[:, i * LANES : (i + 1) * LANES]
            turned = jnp.broadcast_to(moved[:, i * LANES : (i + 1) * LANES], (8, LANES)).T
            sorted_columns[at * LANES : (at + 1) * LANES, :] = jnp.broadcast_to(turned[:, 0:1], (LANES, LANES))

    def rows_of(b, k):
        place = lax.broadcasted_iota(jnp.int32, (BLOCK, LANES), 0) + b * BLOCK
        hit = jnp.concatenate(
            [
                jnp.where(sorted_ids[pl.ds(k + i, 1), :] == place, 1.0, 0.0).astype(x.dtype)
                for i in range(WINDOW // LANES)
            ],
            axis=1,
        )
        at = pl.ds(pl.multiple_of(k * LANES, LANES), WINDOW)
        return jnp.dot(hit, sorted_x[at, :], preferred_element_type=jnp.float32)

    def counts_of(b, k):
        column = sorted_columns[pl.ds(pl.multiple_of(k * LANES, LANES), WINDOW), :].reshape(WINDOW // 8, 8, LANES)
        place = lax.broadcasted_iota(jnp.int32, (1, 1, LANES), 2) + b * BLOCK
        return jnp.concatenate(
            [
                jnp.sum(jnp.sum((column == place + i * LANES).astype(jnp.float32), axis=0), axis=0, keepdims=True)
                for i in range(BLOCK // LANES)
            ],
            axis=0,
        )

    def out_copy(b):
        at = pl.ds(b * BLOCK, min(BLOCK, VOCAB_DEV - b * BLOCK))
        return pltpu.make_async_copy(table.at[at, :], table_hbm.at[at, :], sem.at[b])

    def window_of(b):
        return jnp.minimum(lax.shift_right_logical(starts[b], 7), chunks - 1)

    def build(b):
        k = window_of(b)
        table[b * BLOCK : (b + 1) * BLOCK, :] = rows_of(b, k)
        share[b * (BLOCK // LANES) : (b + 1) * (BLOCK // LANES), :] = counts_of(b, k) * scale
        out_copy(b).start()

    windows = total // WINDOW
    short = jnp.int32(0)
    built = 0
    for c in range(windows):
        order(c)
        ready = BLOCKS if c == windows - 1 else max((c + 1) * BLOCKS // windows - 2, 0)
        for b in range(built, ready):
            build(b)
        if ready > built:
            short = jnp.maximum(short, starts[ready] - (c + 1) * WINDOW)
        built = max(built, ready)
    for b in range(BLOCKS):
        short = jnp.maximum(short, starts[b + 1] - window_of(b) * LANES - WINDOW)

    @pl.when(short > 0)
    def _():
        for b in range(BLOCKS):
            out_copy(b).wait()

        def again(b, _):
            at = pl.ds(pl.multiple_of(b * BLOCK, BLOCK), BLOCK)
            share_at = pl.ds(b * (BLOCK // LANES), BLOCK // LANES)
            table[at, :] = jnp.zeros((BLOCK, table.shape[1]), jnp.float32)
            share[share_at, :] = jnp.zeros((BLOCK // LANES, LANES), jnp.float32)

            def window(w, _):
                k = window_of(b) + w * (WINDOW // LANES)
                table[at, :] += rows_of(b, k)
                share[share_at, :] += counts_of(b, k) * scale
                return 0

            count = lax.div(jnp.maximum(starts[b + 1] - window_of(b) * LANES + WINDOW - 1, 0), WINDOW)
            return lax.fori_loop(0, count, window, 0)

        lax.fori_loop(0, BLOCKS, again, 0)
        for b in range(BLOCKS):
            out_copy(b).start()

    share_copy = pltpu.make_async_copy(share, share_hbm, sem.at[BLOCKS])
    share_copy.start()
    for b in range(BLOCKS):
        out_copy(b).wait()
    share_copy.wait()


def make_table(got, scale):
    sources, length, _ = got.shape
    total = sources * CAP
    chunks = total // LANES
    width = (length - ID_ROWS) // CAP * LANES
    return pl.pallas_call(
        functools.partial(table_kernel, scale),
        out_shape=(
            jax.ShapeDtypeStruct((VOCAB_DEV, width), jnp.float32),
            jax.ShapeDtypeStruct((BLOCKS * BLOCK // LANES, LANES), jnp.float32),
        ),
        in_specs=[pl.BlockSpec(memory_space=pltpu.VMEM)],
        out_specs=(pl.BlockSpec(memory_space=pl.ANY), pl.BlockSpec(memory_space=pl.ANY)),
        scratch_shapes=[
            pltpu.VMEM((total, width), got.dtype),
            pltpu.VMEM((chunks, LANES), jnp.int32),
            pltpu.VMEM((chunks, LANES), jnp.int32),
            pltpu.VMEM((total, LANES), jnp.int32),
            pltpu.VMEM((chunks, LANES), jnp.int32),
            pltpu.VMEM((chunks + 8, LANES), jnp.int32),
            pltpu.VMEM((total + LANES, LANES), jnp.int32),
            pltpu.VMEM((total + LANES, width), got.dtype),
            pltpu.VMEM((BLOCKS * BLOCK, width), jnp.float32),
            pltpu.VMEM((BLOCKS * BLOCK // LANES, LANES), jnp.float32),
            pltpu.SMEM((BLOCKS + 1,), jnp.int32),
            pltpu.SemaphoreType.DMA((BLOCKS + 1,)),
        ],
        compiler_params=pltpu.CompilerParams(vmem_limit_bytes=48 * 1024 * 1024),
        name="table",
    )(got)


def local(grads, token_ids):
    n_vocab = lax.axis_size("vocab")
    n_data = lax.axis_size("dp")
    rows, ids = bucket(token_ids, grads, n_vocab)
    sent = pack(rows, ids, n_vocab, n_data)
    got = lax.all_to_all(sent, AXES, split_axis=0, concat_axis=0, tiled=True)
    table, share = make_table(got, VOCAB_DEV / (TOK_DEV * n_data))
    return table, share.reshape(-1)[:VOCAB_DEV]


def solution(mesh):
    in_specs = (P(AXES, None), P(AXES))
    out_specs = (P("vocab", "dp"), P("vocab"))
    return jax.shard_map(local, mesh=mesh, in_specs=in_specs, out_specs=out_specs, check_vma=False)
```

```python
import functools

import jax
import jax.numpy as jnp
from jax import lax
from jax.experimental import pallas as pl
from jax.experimental.pallas import tpu as pltpu
from jax.sharding import PartitionSpec as P

VOCAB_DEV = 8016
TOK_DEV = 128
CAP = 32
AXES = ("vocab", "dp")
LANES = 128
GROUP = LANES // CAP
ID_ROWS = 8
BLOCK = 512
BLOCKS = -(-VOCAB_DEV // BLOCK)
WINDOW = 256


def bucket(ids, data, n_vocab):
    length = ids.shape[0]
    if n_vocab * CAP == length:
        return data, ids.reshape(1, length)
    owner_start = jnp.arange(n_vocab, dtype=jnp.int32) * VOCAB_DEV
    starts = jnp.sum((ids[None, :] < owner_start[:, None]).astype(jnp.int32), axis=1)
    finish = jnp.concatenate([starts[1:], jnp.full((1,), length, jnp.int32)])
    slot = jnp.arange(CAP, dtype=jnp.int32)
    places = starts[:, None] + slot[None, :]
    valid = places < finish[:, None]
    columns = jnp.arange(length, dtype=jnp.int32)
    select = (places[:, :, None] == columns) & valid[:, :, None]
    rows = jnp.einsum(
        "vcl,ld->vcd", select.astype(data.dtype), data, preferred_element_type=jnp.float32
    ).astype(data.dtype)
    picked = jnp.sum(jnp.where(select, ids, 0), axis=2)
    slot_ids = jnp.where(valid, picked, -1)
    return rows.reshape(n_vocab * CAP, data.shape[1]), slot_ids.reshape(1, n_vocab * CAP)


def pack_kernel(n_vocab, n_data, rows_hbm, ids_ref, out_hbm, rows, out, in_sem, out_sem):
    tiles = rows.shape[1] // (n_data * LANES)
    loads = []
    for v in range(n_vocab):
        strip = pl.ds(v * CAP, CAP)
        loads.append(pltpu.make_async_copy(rows_hbm.at[strip], rows.at[strip], in_sem.at[v]))
        loads[-1].start()
    source = lax.axis_index("vocab") * n_data + lax.axis_index("dp")
    lane = lax.broadcasted_iota(jnp.int32, (ID_ROWS, LANES), 1)
    sub = lax.broadcasted_iota(jnp.int32, (ID_ROWS, LANES), 0)
    row = lax.rem(lax.div(source, GROUP), ID_ROWS // 2)
    here = lax.div(lane, CAP) == lax.rem(source, GROUP)
    stores = []
    for v in range(n_vocab):
        ids = ids_ref[:, v * CAP : (v + 1) * CAP]
        ids = jnp.where(ids < 0, -1, ids - v * VOCAB_DEV)
        ids = jnp.concatenate([ids] * GROUP, axis=1)
        high = lax.shift_right_arithmetic(ids, 7).astype(jnp.float32)
        low = jnp.bitwise_and(ids, 127).astype(jnp.float32)
        coded = jnp.where(here & (sub == row), high, 0.0) + jnp.where(here & (sub == row + ID_ROWS // 2), low, 0.0)
        coded = coded.astype(out.dtype)
        loads[v].wait()
        for d in range(n_data):
            for j in range(tiles):
                column = (d * tiles + j) * LANES
                out[v * n_data + d, j * CAP : (j + 1) * CAP, :] = rows[
                    v * CAP : (v + 1) * CAP, column : column + LANES
                ]
            out[v * n_data + d, tiles * CAP : tiles * CAP + ID_ROWS, :] = coded
        strip = pl.ds(v * n_data, n_data)
        stores.append(pltpu.make_async_copy(out.at[strip], out_hbm.at[strip], out_sem.at[v]))
        stores[-1].start()
    for store in stores:
        store.wait()


def pack(rows, ids, n_vocab, n_data):
    width = rows.shape[1] // n_data
    length = width // LANES * CAP + ID_ROWS
    shape = (n_vocab * n_data, length, LANES)
    return pl.pallas_call(
        functools.partial(pack_kernel, n_vocab, n_data),
        out_shape=jax.ShapeDtypeStruct(shape, rows.dtype),
        in_specs=[pl.BlockSpec(memory_space=pl.ANY), pl.BlockSpec(memory_space=pltpu.VMEM)],
        out_specs=pl.BlockSpec(memory_space=pl.ANY),
        scratch_shapes=[
            pltpu.VMEM(rows.shape, rows.dtype),
            pltpu.VMEM(shape, rows.dtype),
            pltpu.SemaphoreType.DMA((n_vocab,)),
            pltpu.SemaphoreType.DMA((n_vocab,)),
        ],
        name="pack",
    )(rows, ids)


def table_kernel(scale, got, table_hbm, share_hbm, x, ids_s, sorted_ids, sorted_x, table, share, starts, sem):
    sources, length, _ = got.shape
    total = sources * CAP
    chunks = total // LANES
    tiles = (length - ID_ROWS) // CAP
    half = ID_ROWS // 2
    per = half * GROUP
    for g in range(sources // per):
        coded = got[g * per, tiles * CAP :, :].astype(jnp.float32)
        for s in range(g * per + 1, (g + 1) * per):
            coded = coded + got[s, tiles * CAP :, :].astype(jnp.float32)
        ids_s[g * half : (g + 1) * half, :] = (coded[:half] * 128.0 + coded[half:]).astype(jnp.int32)
    ids = ids_s[...]
    ids = jnp.where(ids < 0, BLOCKS * BLOCK, ids)
    for b in range(BLOCKS + 1):
        starts[b] = jnp.sum((ids < b * BLOCK).astype(jnp.int32))
    for j in range(tiles):
        x[:, j * LANES : (j + 1) * LANES] = got[:, j * CAP : (j + 1) * CAP, :].reshape(total, LANES)
    sorted_ids[...] = jnp.full(sorted_ids.shape, -1, jnp.int32)
    sorted_x[...] = jnp.zeros(sorted_x.shape, x.dtype)

    block = lax.div(ids, BLOCK)
    inside = [jnp.where(block == b, 1.0, 0.0) for b in range(BLOCKS)]
    mask = jnp.concatenate(inside, axis=0).astype(x.dtype)
    above = lax.broadcasted_iota(jnp.int32, (LANES, 2 * LANES), 0) < lax.broadcasted_iota(
        jnp.int32, (LANES, 2 * LANES), 1
    )
    ahead = jnp.dot(mask, jnp.where(above, 1.0, 0.0).astype(x.dtype), preferred_element_type=jnp.float32)
    groups = BLOCKS * chunks
    below = lax.broadcasted_iota(jnp.int32, (groups, groups), 0) > lax.broadcasted_iota(jnp.int32, (groups, groups), 1)
    earlier = jnp.dot(
        jnp.where(below, 1.0, 0.0).astype(x.dtype), ahead[:, LANES:].astype(x.dtype), preferred_element_type=jnp.float32
    )
    ahead = ahead[:, :LANES] + earlier
    place = jnp.where(block < BLOCKS, 0.0, float(total))
    for b in range(BLOCKS):
        place = place + inside[b] * ahead[b * chunks : (b + 1) * chunks]
    place = place.astype(jnp.int32)

    flat = jnp.concatenate([ids[p : p + 1, :] for p in range(chunks)], axis=1)
    pick = lax.broadcasted_iota(jnp.int32, (8, total), 0)
    parts = jnp.where(pick == 0, lax.shift_right_arithmetic(flat, 7), jnp.bitwise_and(flat, 127))
    parts = parts.astype(jnp.float32).astype(x.dtype)

    def order(c):
        at = lax.broadcasted_iota(jnp.int32, (WINDOW, LANES), 0) + c * WINDOW
        move = jnp.concatenate(
            [jnp.where(place[p : p + 1, :] == at, 1.0, 0.0).astype(x.dtype) for p in range(chunks)], axis=1
        )
        moved = lax.dot_general(parts, move, (((1,), (1,)), ((), ())), preferred_element_type=jnp.float32)
        moved = (moved[0:1] * 128.0 + moved[1:2]).astype(jnp.int32)
        for i in range(WINDOW // LANES):
            row = c * (WINDOW // LANES) + i
            sorted_ids[row : row + 1, :] = moved[:, i * LANES : (i + 1) * LANES]
        sorted_x[c * WINDOW : (c + 1) * WINDOW, :] = jnp.dot(
            move, x[...], preferred_element_type=jnp.float32
        ).astype(x.dtype)

    def rows_of(b, k):
        row = lax.broadcasted_iota(jnp.int32, (BLOCK, LANES), 0) + b * BLOCK
        hit = jnp.concatenate(
            [
                jnp.where(sorted_ids[pl.ds(k + i, 1), :] == row, 1.0, 0.0).astype(x.dtype)
                for i in range(WINDOW // LANES)
            ],
            axis=1,
        )
        at = pl.ds(pl.multiple_of(k * LANES, LANES), WINDOW)
        return jnp.dot(hit, sorted_x[at, :], preferred_element_type=jnp.float32)

    def out_copy(b):
        at = pl.ds(b * BLOCK, min(BLOCK, VOCAB_DEV - b * BLOCK))
        return pltpu.make_async_copy(table.at[at, :], table_hbm.at[at, :], sem.at[b])

    def window_of(b):
        return jnp.minimum(lax.shift_right_logical(starts[b], 7), chunks - 1)

    windows = total // WINDOW
    short = jnp.int32(0)
    built = 0
    for c in range(windows):
        order(c)
        ready = BLOCKS if c == windows - 1 else max((c + 1) * BLOCKS // windows - 2, 0)
        for b in range(built, ready):
            table[b * BLOCK : (b + 1) * BLOCK, :] = rows_of(b, window_of(b))
            out_copy(b).start()
        if ready > built:
            short = jnp.maximum(short, starts[ready] - (c + 1) * WINDOW)
        built = max(built, ready)
    for b in range(BLOCKS):
        short = jnp.maximum(short, starts[b + 1] - window_of(b) * LANES - WINDOW)

    def spread(size, value):
        of = lax.broadcasted_iota(jnp.int32, (size, LANES), 0)
        return jnp.concatenate(
            [jnp.where(value[p : p + 1, :] == of, 1.0, 0.0).astype(x.dtype) for p in range(chunks)], axis=1
        )

    share[...] = scale * lax.dot_general(
        spread(BLOCKS * BLOCK // LANES, lax.shift_right_arithmetic(ids, 7)),
        spread(LANES, jnp.bitwise_and(ids, 127)),
        (((1,), (1,)), ((), ())),
        preferred_element_type=jnp.float32,
    )
    share_copy = pltpu.make_async_copy(share, share_hbm, sem.at[BLOCKS])
    share_copy.start()

    @pl.when(short > 0)
    def _():
        for b in range(BLOCKS):
            out_copy(b).wait()

        def again(b, _):
            at = pl.ds(pl.multiple_of(b * BLOCK, BLOCK), BLOCK)
            table[at, :] = jnp.zeros((BLOCK, table.shape[1]), jnp.float32)

            def window(w, _):
                table[at, :] += rows_of(b, window_of(b) + w * (WINDOW // LANES))
                return 0

            count = lax.div(jnp.maximum(starts[b + 1] - window_of(b) * LANES + WINDOW - 1, 0), WINDOW)
            return lax.fori_loop(0, count, window, 0)

        lax.fori_loop(0, BLOCKS, again, 0)
        for b in range(BLOCKS):
            out_copy(b).start()

    for b in range(BLOCKS):
        out_copy(b).wait()
    share_copy.wait()


def make_table(got, scale):
    sources, length, _ = got.shape
    total = sources * CAP
    chunks = total // LANES
    width = (length - ID_ROWS) // CAP * LANES
    return pl.pallas_call(
        functools.partial(table_kernel, scale),
        out_shape=(
            jax.ShapeDtypeStruct((VOCAB_DEV, width), jnp.float32),
            jax.ShapeDtypeStruct((BLOCKS * BLOCK // LANES, LANES), jnp.float32),
        ),
        in_specs=[pl.BlockSpec(memory_space=pltpu.VMEM)],
        out_specs=(pl.BlockSpec(memory_space=pl.ANY), pl.BlockSpec(memory_space=pl.ANY)),
        scratch_shapes=[
            pltpu.VMEM((total, width), got.dtype),
            pltpu.VMEM((chunks, LANES), jnp.int32),
            pltpu.VMEM((chunks + 8, LANES), jnp.int32),
            pltpu.VMEM((total + LANES, width), got.dtype),
            pltpu.VMEM((BLOCKS * BLOCK, width), jnp.float32),
            pltpu.VMEM((BLOCKS * BLOCK // LANES, LANES), jnp.float32),
            pltpu.SMEM((BLOCKS + 1,), jnp.int32),
            pltpu.SemaphoreType.DMA((BLOCKS + 1,)),
        ],
        compiler_params=pltpu.CompilerParams(vmem_limit_bytes=48 * 1024 * 1024),
        name="table",
    )(got)


def local(grads, token_ids):
    n_vocab = lax.axis_size("vocab")
    n_data = lax.axis_size("dp")
    rows, ids = bucket(token_ids, grads, n_vocab)
    sent = pack(rows, ids, n_vocab, n_data)
    got = lax.all_to_all(sent, AXES, split_axis=0, concat_axis=0, tiled=True)
    table, share = make_table(got, VOCAB_DEV / (TOK_DEV * n_data))
    return table, share.reshape(-1)[:VOCAB_DEV]


def solution(mesh):
    in_specs = (P(AXES, None), P(AXES))
    out_specs = (P("vocab", "dp"), P("vocab"))
    return jax.shard_map(local, mesh=mesh, in_specs=in_specs, out_specs=out_specs, check_vma=False)
```

```python
import functools

import jax
import jax.numpy as jnp
from jax import lax
from jax.experimental import pallas as pl
from jax.experimental.pallas import tpu as pltpu
from jax.sharding import PartitionSpec as P

VOCAB_DEV = 8016
TOK_DEV = 128
CAP = 32
AXES = ("vocab", "dp")
LANES = 128
GROUP = LANES // CAP
ID_ROWS = 8
BLOCK = 512
BLOCKS = -(-VOCAB_DEV // BLOCK)
WINDOW = 256


def bucket(ids, data, n_vocab):
    length = ids.shape[0]
    if n_vocab * CAP == length:
        return data, ids.reshape(1, length)
    owner_start = jnp.arange(n_vocab, dtype=jnp.int32) * VOCAB_DEV
    starts = jnp.sum((ids[None, :] < owner_start[:, None]).astype(jnp.int32), axis=1)
    finish = jnp.concatenate([starts[1:], jnp.full((1,), length, jnp.int32)])
    slot = jnp.arange(CAP, dtype=jnp.int32)
    places = starts[:, None] + slot[None, :]
    valid = places < finish[:, None]
    columns = jnp.arange(length, dtype=jnp.int32)
    select = (places[:, :, None] == columns) & valid[:, :, None]
    rows = jnp.einsum(
        "vcl,ld->vcd", select.astype(data.dtype), data, preferred_element_type=jnp.float32
    ).astype(data.dtype)
    picked = jnp.sum(jnp.where(select, ids, 0), axis=2)
    slot_ids = jnp.where(valid, picked, -1)
    return rows.reshape(n_vocab * CAP, data.shape[1]), slot_ids.reshape(1, n_vocab * CAP)


def pack_kernel(n_vocab, n_data, rows_hbm, ids_hbm, out_hbm, rows, ids_ref, out, in_sem, out_sem):
    tiles = rows.shape[1] // (n_data * LANES)
    ids_copy = pltpu.make_async_copy(ids_hbm, ids_ref, in_sem.at[n_vocab])
    ids_copy.start()
    loads = []
    for v in range(n_vocab):
        strip = pl.ds(v * CAP, CAP)
        loads.append(pltpu.make_async_copy(rows_hbm.at[strip], rows.at[strip], in_sem.at[v]))
        loads[-1].start()
    source = lax.axis_index("vocab") * n_data + lax.axis_index("dp")
    lane = lax.broadcasted_iota(jnp.int32, (ID_ROWS, LANES), 1)
    sub = lax.broadcasted_iota(jnp.int32, (ID_ROWS, LANES), 0)
    row = lax.rem(lax.div(source, GROUP), ID_ROWS // 2)
    here = lax.div(lane, CAP) == lax.rem(source, GROUP)
    stores = []
    ids_copy.wait()
    for v in range(n_vocab):
        ids = ids_ref[:, v * CAP : (v + 1) * CAP]
        ids = jnp.where(ids < 0, -1, ids - v * VOCAB_DEV)
        ids = jnp.concatenate([ids] * GROUP, axis=1)
        high = lax.shift_right_arithmetic(ids, 7).astype(jnp.float32)
        low = jnp.bitwise_and(ids, 127).astype(jnp.float32)
        coded = jnp.where(here & (sub == row), high, 0.0) + jnp.where(here & (sub == row + ID_ROWS // 2), low, 0.0)
        coded = coded.astype(out.dtype)
        loads[v].wait()
        for d in range(n_data):
            for j in range(tiles):
                column = (d * tiles + j) * LANES
                out[v * n_data + d, j * CAP : (j + 1) * CAP, :] = rows[
                    v * CAP : (v + 1) * CAP, column : column + LANES
                ]
            out[v * n_data + d, tiles * CAP : tiles * CAP + ID_ROWS, :] = coded
        strip = pl.ds(v * n_data, n_data)
        stores.append(pltpu.make_async_copy(out.at[strip], out_hbm.at[strip], out_sem.at[v]))
        stores[-1].start()
    for store in stores:
        store.wait()


def pack(rows, ids, n_vocab, n_data):
    width = rows.shape[1] // n_data
    length = width // LANES * CAP + ID_ROWS
    shape = (n_vocab * n_data, length, LANES)
    return pl.pallas_call(
        functools.partial(pack_kernel, n_vocab, n_data),
        out_shape=jax.ShapeDtypeStruct(shape, rows.dtype),
        in_specs=[pl.BlockSpec(memory_space=pl.ANY)] * 2,
        out_specs=pl.BlockSpec(memory_space=pl.ANY),
        scratch_shapes=[
            pltpu.VMEM(rows.shape, rows.dtype),
            pltpu.VMEM(ids.shape, ids.dtype),
            pltpu.VMEM(shape, rows.dtype),
            pltpu.SemaphoreType.DMA((n_vocab + 1,)),
            pltpu.SemaphoreType.DMA((n_vocab,)),
        ],
        name="pack",
    )(rows, ids)


def table_kernel(scale, got, table_hbm, share_hbm, x, ids_s, sorted_ids, sorted_x, table, share, starts, sem):
    sources, length, _ = got.shape
    total = sources * CAP
    chunks = total // LANES
    tiles = (length - ID_ROWS) // CAP
    half = ID_ROWS // 2
    per = half * GROUP
    for g in range(sources // per):
        coded = got[g * per, tiles * CAP :, :].astype(jnp.float32)
        for s in range(g * per + 1, (g + 1) * per):
            coded = coded + got[s, tiles * CAP :, :].astype(jnp.float32)
        ids_s[g * half : (g + 1) * half, :] = (coded[:half] * 128.0 + coded[half:]).astype(jnp.int32)
    ids = ids_s[...]
    ids = jnp.where(ids < 0, BLOCKS * BLOCK, ids)
    for b in range(BLOCKS + 1):
        starts[b] = jnp.sum((ids < b * BLOCK).astype(jnp.int32))
    for j in range(tiles):
        x[:, j * LANES : (j + 1) * LANES] = got[:, j * CAP : (j + 1) * CAP, :].reshape(total, LANES)
    sorted_ids[...] = jnp.full(sorted_ids.shape, -1, jnp.int32)
    sorted_x[...] = jnp.zeros(sorted_x.shape, x.dtype)

    block = lax.div(ids, BLOCK)
    inside = [jnp.where(block == b, 1.0, 0.0) for b in range(BLOCKS)]
    mask = jnp.concatenate(inside, axis=0).astype(x.dtype)
    above = lax.broadcasted_iota(jnp.int32, (LANES, 2 * LANES), 0) < lax.broadcasted_iota(
        jnp.int32, (LANES, 2 * LANES), 1
    )
    ahead = jnp.dot(mask, jnp.where(above, 1.0, 0.0).astype(x.dtype), preferred_element_type=jnp.float32)
    groups = BLOCKS * chunks
    below = lax.broadcasted_iota(jnp.int32, (groups, groups), 0) > lax.broadcasted_iota(jnp.int32, (groups, groups), 1)
    earlier = jnp.dot(
        jnp.where(below, 1.0, 0.0).astype(x.dtype), ahead[:, LANES:].astype(x.dtype), preferred_element_type=jnp.float32
    )
    ahead = ahead[:, :LANES] + earlier
    place = jnp.where(block < BLOCKS, 0.0, float(total))
    for b in range(BLOCKS):
        place = place + inside[b] * ahead[b * chunks : (b + 1) * chunks]
    place = place.astype(jnp.int32)

    flat = jnp.concatenate([ids[p : p + 1, :] for p in range(chunks)], axis=1)
    pick = lax.broadcasted_iota(jnp.int32, (8, total), 0)
    parts = jnp.where(pick == 0, lax.shift_right_arithmetic(flat, 7), jnp.bitwise_and(flat, 127))
    parts = parts.astype(jnp.float32).astype(x.dtype)

    def order(c):
        at = lax.broadcasted_iota(jnp.int32, (WINDOW, LANES), 0) + c * WINDOW
        move = jnp.concatenate(
            [jnp.where(place[p : p + 1, :] == at, 1.0, 0.0).astype(x.dtype) for p in range(chunks)], axis=1
        )
        moved = lax.dot_general(parts, move, (((1,), (1,)), ((), ())), preferred_element_type=jnp.float32)
        moved = (moved[0:1] * 128.0 + moved[1:2]).astype(jnp.int32)
        for i in range(WINDOW // LANES):
            row = c * (WINDOW // LANES) + i
            sorted_ids[row : row + 1, :] = moved[:, i * LANES : (i + 1) * LANES]
        sorted_x[c * WINDOW : (c + 1) * WINDOW, :] = jnp.dot(
            move, x[...], preferred_element_type=jnp.float32
        ).astype(x.dtype)

    def rows_of(b, k):
        row = lax.broadcasted_iota(jnp.int32, (BLOCK, LANES), 0) + b * BLOCK
        hit = jnp.concatenate(
            [
                jnp.where(sorted_ids[pl.ds(k + i, 1), :] == row, 1.0, 0.0).astype(x.dtype)
                for i in range(WINDOW // LANES)
            ],
            axis=1,
        )
        at = pl.ds(pl.multiple_of(k * LANES, LANES), WINDOW)
        return jnp.dot(hit, sorted_x[at, :], preferred_element_type=jnp.float32)

    def out_copy(b):
        at = pl.ds(b * BLOCK, min(BLOCK, VOCAB_DEV - b * BLOCK))
        return pltpu.make_async_copy(table.at[at, :], table_hbm.at[at, :], sem.at[b])

    def window_of(b):
        return jnp.minimum(lax.shift_right_logical(starts[b], 7), chunks - 1)

    windows = total // WINDOW
    short = jnp.int32(0)
    built = 0
    for c in range(windows):
        order(c)
        ready = BLOCKS if c == windows - 1 else max((c + 1) * BLOCKS // windows - 2, 0)
        for b in range(built, ready):
            table[b * BLOCK : (b + 1) * BLOCK, :] = rows_of(b, window_of(b))
            out_copy(b).start()
        if ready > built:
            short = jnp.maximum(short, starts[ready] - (c + 1) * WINDOW)
        built = max(built, ready)
    for b in range(BLOCKS):
        short = jnp.maximum(short, starts[b + 1] - window_of(b) * LANES - WINDOW)

    def spread(size, value):
        of = lax.broadcasted_iota(jnp.int32, (size, LANES), 0)
        return jnp.concatenate(
            [jnp.where(value[p : p + 1, :] == of, 1.0, 0.0).astype(x.dtype) for p in range(chunks)], axis=1
        )

    share[...] = scale * lax.dot_general(
        spread(BLOCKS * BLOCK // LANES, lax.shift_right_arithmetic(ids, 7)),
        spread(LANES, jnp.bitwise_and(ids, 127)),
        (((1,), (1,)), ((), ())),
        preferred_element_type=jnp.float32,
    )
    share_copy = pltpu.make_async_copy(share, share_hbm, sem.at[BLOCKS])
    share_copy.start()

    @pl.when(short > 0)
    def _():
        for b in range(BLOCKS):
            out_copy(b).wait()

        def again(b, _):
            at = pl.ds(pl.multiple_of(b * BLOCK, BLOCK), BLOCK)
            table[at, :] = jnp.zeros((BLOCK, table.shape[1]), jnp.float32)

            def window(w, _):
                table[at, :] += rows_of(b, window_of(b) + w * (WINDOW // LANES))
                return 0

            count = lax.div(jnp.maximum(starts[b + 1] - window_of(b) * LANES + WINDOW - 1, 0), WINDOW)
            return lax.fori_loop(0, count, window, 0)

        lax.fori_loop(0, BLOCKS, again, 0)
        for b in range(BLOCKS):
            out_copy(b).start()

    for b in range(BLOCKS):
        out_copy(b).wait()
    share_copy.wait()


def make_table(got, scale):
    sources, length, _ = got.shape
    total = sources * CAP
    chunks = total // LANES
    width = (length - ID_ROWS) // CAP * LANES
    return pl.pallas_call(
        functools.partial(table_kernel, scale),
        out_shape=(
            jax.ShapeDtypeStruct((VOCAB_DEV, width), jnp.float32),
            jax.ShapeDtypeStruct((BLOCKS * BLOCK // LANES, LANES), jnp.float32),
        ),
        in_specs=[pl.BlockSpec(memory_space=pltpu.VMEM)],
        out_specs=(pl.BlockSpec(memory_space=pl.ANY), pl.BlockSpec(memory_space=pl.ANY)),
        scratch_shapes=[
            pltpu.VMEM((total, width), got.dtype),
            pltpu.VMEM((chunks, LANES), jnp.int32),
            pltpu.VMEM((chunks + 8, LANES), jnp.int32),
            pltpu.VMEM((total + LANES, width), got.dtype),
            pltpu.VMEM((BLOCKS * BLOCK, width), jnp.float32),
            pltpu.VMEM((BLOCKS * BLOCK // LANES, LANES), jnp.float32),
            pltpu.SMEM((BLOCKS + 1,), jnp.int32),
            pltpu.SemaphoreType.DMA((BLOCKS + 1,)),
        ],
        compiler_params=pltpu.CompilerParams(vmem_limit_bytes=48 * 1024 * 1024),
        name="table",
    )(got)


def local(grads, token_ids):
    n_vocab = lax.axis_size("vocab")
    n_data = lax.axis_size("dp")
    rows, ids = bucket(token_ids, grads, n_vocab)
    sent = pack(rows, ids, n_vocab, n_data)
    got = lax.all_to_all(sent, AXES, split_axis=0, concat_axis=0, tiled=True)
    table, share = make_table(got, VOCAB_DEV / (TOK_DEV * n_data))
    return table, share.reshape(-1)[:VOCAB_DEV]


def solution(mesh):
    in_specs = (P(AXES, None), P(AXES))
    out_specs = (P("vocab", "dp"), P("vocab"))
    return jax.shard_map(local, mesh=mesh, in_specs=in_specs, out_specs=out_specs, check_vma=False)
```

```python
import functools

import jax
import jax.numpy as jnp
from jax import lax
from jax.experimental import pallas as pl
from jax.experimental.pallas import tpu as pltpu
from jax.sharding import PartitionSpec as P


VOCAB_DEV = 8016
TOK_DEV = 128
CAP = 32
AXES = ("vocab", "dp")
LANES = 128
GROUP = LANES // CAP
BLOCK = 512
BLOCKS = -(-VOCAB_DEV // BLOCK)
WINDOW = 256


def bucket(ids, data, n_vocab):
    length = ids.shape[0]
    if n_vocab * CAP == length:
        return data, ids.reshape(1, length)
    owner_start = jnp.arange(n_vocab, dtype=jnp.int32) * VOCAB_DEV
    starts = jnp.sum((ids[None, :] < owner_start[:, None]).astype(jnp.int32), axis=1)
    finish = jnp.concatenate([starts[1:], jnp.full((1,), length, jnp.int32)])
    slot = jnp.arange(CAP, dtype=jnp.int32)
    places = starts[:, None] + slot[None, :]
    valid = places < finish[:, None]
    columns = jnp.arange(length, dtype=jnp.int32)
    select = (places[:, :, None] == columns) & valid[:, :, None]
    rows = jnp.einsum(
        "vcl,ld->vcd", select.astype(data.dtype), data, preferred_element_type=jnp.float32
    ).astype(data.dtype)
    picked = jnp.sum(jnp.where(select, ids, 0), axis=2)
    slot_ids = jnp.where(valid, picked, -1)
    return rows.reshape(n_vocab * CAP, data.shape[1]), slot_ids.reshape(1, n_vocab * CAP)


def pack_kernel(n_vocab, n_data, rows_hbm, out_hbm, rows, out, in_sem, out_sem):
    tiles = rows.shape[1] // (n_data * LANES)
    loads = []
    for v in range(n_vocab):
        strip = pl.ds(v * CAP, CAP)
        loads.append(pltpu.make_async_copy(rows_hbm.at[strip], rows.at[strip], in_sem.at[v]))
        loads[-1].start()
    stores = []
    for v in range(n_vocab):
        loads[v].wait()
        for d in range(n_data):
            for j in range(tiles):
                column = (d * tiles + j) * LANES
                out[v * n_data + d, j * CAP : (j + 1) * CAP, :] = rows[
                    v * CAP : (v + 1) * CAP, column : column + LANES
                ]
        strip = pl.ds(v * n_data, n_data)
        stores.append(pltpu.make_async_copy(out.at[strip], out_hbm.at[strip], out_sem.at[v]))
        stores[-1].start()
    for store in stores:
        store.wait()


def pack(rows, n_vocab, n_data):
    shape = (n_vocab * n_data, rows.shape[1] // (n_data * LANES) * CAP, LANES)
    return pl.pallas_call(
        functools.partial(pack_kernel, n_vocab, n_data),
        out_shape=jax.ShapeDtypeStruct(shape, rows.dtype),
        in_specs=[pl.BlockSpec(memory_space=pl.ANY)],
        out_specs=pl.BlockSpec(memory_space=pl.ANY),
        scratch_shapes=[
            pltpu.VMEM(rows.shape, rows.dtype),
            pltpu.VMEM(shape, rows.dtype),
            pltpu.SemaphoreType.DMA((n_vocab,)),
            pltpu.SemaphoreType.DMA((n_vocab,)),
        ],
        name="pack",
    )(rows)


def exchange_ids(ids, n_vocab, n_data):
    def from_device(x, apart):
        return lax.ppermute(x, AXES, [(i, i ^ apart) for i in range(n_vocab * n_data)])

    ids = jnp.concatenate([ids, from_device(ids, 1)])
    ids = jnp.concatenate([ids] + [from_device(ids, v * n_data) for v in range(1, n_vocab)])
    return [ids] + [from_device(ids, z) for z in range(2, n_data, 2)]


def table_kernel(scale, n_vocab, n_data, got, *refs):
    parts_in = refs[: n_data // 2]
    table_hbm, share_hbm, x, ids_s, sorted_ids, sorted_x, table, share, starts, sem = refs[n_data // 2 :]
    sources, length, _ = got.shape
    total = sources * CAP
    chunks = total // LANES
    tiles = length // CAP
    vocab, data = lax.axis_index("vocab"), lax.axis_index("dp")
    near = 2 * n_vocab
    lane = lax.broadcasted_iota(jnp.int32, (near, LANES), 1)
    sub = lax.broadcasted_iota(jnp.int32, (near, LANES), 0)
    here = lax.div(lane, CAP) == lax.rem(sub, GROUP)
    for z in range(n_data // 2):
        mine = parts_in[z][:, :CAP]
        for v in range(1, n_vocab):
            mine = jnp.where(vocab == v, parts_in[z][:, v * CAP : (v + 1) * CAP], mine)
        mine = jnp.where(here, jnp.concatenate([mine] * GROUP, axis=1), 0)
        for i in range(near // GROUP):
            row = z * (near // GROUP) + i
            ids_s[row : row + 1, :] = jnp.sum(mine[i * GROUP : (i + 1) * GROUP], axis=0, keepdims=True)
    ids = ids_s[...]
    ids = jnp.where(ids < 0, BLOCKS * BLOCK, ids - vocab * VOCAB_DEV)
    for b in range(BLOCKS + 1):
        starts[b] = jnp.sum((ids < b * BLOCK).astype(jnp.int32))
    for z in range(n_data // 2):
        for v in range(n_vocab):
            for c in range(2):
                source = jnp.bitwise_xor(vocab, v) * n_data + jnp.bitwise_xor(data, 2 * z + c)
                at = ((z * n_vocab + v) * 2 + c) * CAP
                for j in range(tiles):
                    x[at : at + CAP, j * LANES : (j + 1) * LANES] = got[source, j * CAP : (j + 1) * CAP, :]
    sorted_ids[...] = jnp.full(sorted_ids.shape, -1, jnp.int32)
    sorted_x[...] = jnp.zeros(sorted_x.shape, x.dtype)

    block = lax.div(ids, BLOCK)
    inside = [jnp.where(block == b, 1.0, 0.0) for b in range(BLOCKS)]
    mask = jnp.concatenate(inside, axis=0).astype(x.dtype)
    above = lax.broadcasted_iota(jnp.int32, (LANES, 2 * LANES), 0) < lax.broadcasted_iota(
        jnp.int32, (LANES, 2 * LANES), 1
    )
    ahead = jnp.dot(mask, jnp.where(above, 1.0, 0.0).astype(x.dtype), preferred_element_type=jnp.float32)
    groups = BLOCKS * chunks
    below = lax.broadcasted_iota(jnp.int32, (groups, groups), 0) > lax.broadcasted_iota(jnp.int32, (groups, groups), 1)
    earlier = jnp.dot(
        jnp.where(below, 1.0, 0.0).astype(x.dtype), ahead[:, LANES:].astype(x.dtype), preferred_element_type=jnp.float32
    )
    ahead = ahead[:, :LANES] + earlier
    place = jnp.where(block < BLOCKS, 0.0, float(total))
    for b in range(BLOCKS):
        place = place + inside[b] * ahead[b * chunks : (b + 1) * chunks]
    place = place.astype(jnp.int32)

    flat = jnp.concatenate([ids[p : p + 1, :] for p in range(chunks)], axis=1)
    pick = lax.broadcasted_iota(jnp.int32, (8, total), 0)
    parts = jnp.where(pick == 0, lax.shift_right_arithmetic(flat, 7), jnp.bitwise_and(flat, 127))
    parts = parts.astype(jnp.float32).astype(x.dtype)

    def order(c):
        at = lax.broadcasted_iota(jnp.int32, (WINDOW, LANES), 0) + c * WINDOW
        move = jnp.concatenate(
            [jnp.where(place[p : p + 1, :] == at, 1.0, 0.0).astype(x.dtype) for p in range(chunks)], axis=1
        )
        moved = lax.dot_general(parts, move, (((1,), (1,)), ((), ())), preferred_element_type=jnp.float32)
        moved = (moved[0:1] * 128.0 + moved[1:2]).astype(jnp.int32)
        for i in range(WINDOW // LANES):
            row = c * (WINDOW // LANES) + i
            sorted_ids[row : row + 1, :] = moved[:, i * LANES : (i + 1) * LANES]
        sorted_x[c * WINDOW : (c + 1) * WINDOW, :] = jnp.dot(
            move, x[...], preferred_element_type=jnp.float32
        ).astype(x.dtype)

    def rows_of(b, k):
        row = lax.broadcasted_iota(jnp.int32, (BLOCK, LANES), 0) + b * BLOCK
        hit = jnp.concatenate(
            [
                jnp.where(sorted_ids[pl.ds(k + i, 1), :] == row, 1.0, 0.0).astype(x.dtype)
                for i in range(WINDOW // LANES)
            ],
            axis=1,
        )
        at = pl.ds(pl.multiple_of(k * LANES, LANES), WINDOW)
        return jnp.dot(hit, sorted_x[at, :], preferred_element_type=jnp.float32)

    def out_copy(b):
        at = pl.ds(b * BLOCK, min(BLOCK, VOCAB_DEV - b * BLOCK))
        return pltpu.make_async_copy(table.at[at, :], table_hbm.at[at, :], sem.at[b])

    def window_of(b):
        return jnp.minimum(lax.shift_right_logical(starts[b], 7), chunks - 1)

    windows = total // WINDOW
    short = jnp.int32(0)
    built = 0
    for c in range(windows):
        order(c)
        ready = BLOCKS if c == windows - 1 else max((c + 1) * BLOCKS // windows - 2, 0)
        for b in range(built, ready):
            table[b * BLOCK : (b + 1) * BLOCK, :] = rows_of(b, window_of(b))
            out_copy(b).start()
        if ready > built:
            short = jnp.maximum(short, starts[ready] - (c + 1) * WINDOW)
        built = max(built, ready)
    for b in range(BLOCKS):
        short = jnp.maximum(short, starts[b + 1] - window_of(b) * LANES - WINDOW)

    def spread(size, value):
        of = lax.broadcasted_iota(jnp.int32, (size, LANES), 0)
        return jnp.concatenate(
            [jnp.where(value[p : p + 1, :] == of, 1.0, 0.0).astype(x.dtype) for p in range(chunks)], axis=1
        )

    share[...] = scale * lax.dot_general(
        spread(BLOCKS * BLOCK // LANES, lax.shift_right_arithmetic(ids, 7)),
        spread(LANES, jnp.bitwise_and(ids, 127)),
        (((1,), (1,)), ((), ())),
        preferred_element_type=jnp.float32,
    )
    share_copy = pltpu.make_async_copy(share, share_hbm, sem.at[BLOCKS])
    share_copy.start()

    @pl.when(short > 0)
    def _():
        for b in range(BLOCKS):
            out_copy(b).wait()

        def again(b, _):
            at = pl.ds(pl.multiple_of(b * BLOCK, BLOCK), BLOCK)
            table[at, :] = jnp.zeros((BLOCK, table.shape[1]), jnp.float32)

            def window(w, _):
                table[at, :] += rows_of(b, window_of(b) + w * (WINDOW // LANES))
                return 0

            count = lax.div(jnp.maximum(starts[b + 1] - window_of(b) * LANES + WINDOW - 1, 0), WINDOW)
            return lax.fori_loop(0, count, window, 0)

        lax.fori_loop(0, BLOCKS, again, 0)
        for b in range(BLOCKS):
            out_copy(b).start()

    for b in range(BLOCKS):
        out_copy(b).wait()
    share_copy.wait()


def make_table(got, ids, scale, n_vocab, n_data):
    sources, length, _ = got.shape
    total = sources * CAP
    chunks = total // LANES
    width = length // CAP * LANES
    return pl.pallas_call(
        functools.partial(table_kernel, scale, n_vocab, n_data),
        out_shape=(
            jax.ShapeDtypeStruct((VOCAB_DEV, width), jnp.float32),
            jax.ShapeDtypeStruct((BLOCKS * BLOCK // LANES, LANES), jnp.float32),
        ),
        in_specs=[pl.BlockSpec(memory_space=pltpu.VMEM)] * (1 + len(ids)),
        out_specs=(pl.BlockSpec(memory_space=pl.ANY), pl.BlockSpec(memory_space=pl.ANY)),
        scratch_shapes=[
            pltpu.VMEM((total, width), got.dtype),
            pltpu.VMEM((chunks, LANES), jnp.int32),
            pltpu.VMEM((chunks + 8, LANES), jnp.int32),
            pltpu.VMEM((total + LANES, width), got.dtype),
            pltpu.VMEM((BLOCKS * BLOCK, width), jnp.float32),
            pltpu.VMEM((BLOCKS * BLOCK // LANES, LANES), jnp.float32),
            pltpu.SMEM((BLOCKS + 1,), jnp.int32),
            pltpu.SemaphoreType.DMA((BLOCKS + 1,)),
        ],
        compiler_params=pltpu.CompilerParams(vmem_limit_bytes=48 * 1024 * 1024),
        name="table",
    )(got, *ids)


def local(grads, token_ids):
    n_vocab = lax.axis_size("vocab")
    n_data = lax.axis_size("dp")
    rows, ids = bucket(token_ids, grads, n_vocab)
    got = lax.all_to_all(pack(rows, n_vocab, n_data), AXES, split_axis=0, concat_axis=0, tiled=True)
    ids = exchange_ids(ids, n_vocab, n_data)
    table, share = make_table(got, ids, VOCAB_DEV / (TOK_DEV * n_data), n_vocab, n_data)
    return table, share.reshape(-1)[:VOCAB_DEV]


def solution(mesh):
    in_specs = (P(AXES, None), P(AXES))
    out_specs = (P("vocab", "dp"), P("vocab"))
    return jax.shard_map(local, mesh=mesh, in_specs=in_specs, out_specs=out_specs, check_vma=False)
```

```python
import functools

import jax
import jax.numpy as jnp
from jax import lax
from jax.experimental import pallas as pl
from jax.experimental.pallas import tpu as pltpu
from jax.sharding import PartitionSpec as P


VOCAB_DEV = 8016
TOK_DEV = 128
CAP = 32
AXES = ("vocab", "dp")
LANES = 128
GROUP = LANES // CAP
BLOCK = 512
BLOCKS = -(-VOCAB_DEV // BLOCK)
WINDOW = 256


def bucket(ids, data, n_vocab):
    length = ids.shape[0]
    if n_vocab * CAP == length:
        return data, ids.reshape(1, length)
    owner_start = jnp.arange(n_vocab, dtype=jnp.int32) * VOCAB_DEV
    starts = jnp.sum((ids[None, :] < owner_start[:, None]).astype(jnp.int32), axis=1)
    finish = jnp.concatenate([starts[1:], jnp.full((1,), length, jnp.int32)])
    slot = jnp.arange(CAP, dtype=jnp.int32)
    places = starts[:, None] + slot[None, :]
    valid = places < finish[:, None]
    columns = jnp.arange(length, dtype=jnp.int32)
    select = (places[:, :, None] == columns) & valid[:, :, None]
    rows = jnp.einsum(
        "vcl,ld->vcd", select.astype(data.dtype), data, preferred_element_type=jnp.float32
    ).astype(data.dtype)
    picked = jnp.sum(jnp.where(select, ids, 0), axis=2)
    slot_ids = jnp.where(valid, picked, -1)
    return rows.reshape(n_vocab * CAP, data.shape[1]), slot_ids.reshape(1, n_vocab * CAP)


def pack_kernel(n_vocab, n_data, rows_hbm, out_hbm, rows, out, in_sem, out_sem):
    tiles = rows.shape[1] // (n_data * LANES)
    loads = []
    for v in range(n_vocab):
        strip = pl.ds(v * CAP, CAP)
        loads.append(pltpu.make_async_copy(rows_hbm.at[strip], rows.at[strip], in_sem.at[v]))
        loads[-1].start()
    stores = []
    for v in range(n_vocab):
        loads[v].wait()
        for d in range(n_data):
            for j in range(tiles):
                column = (d * tiles + j) * LANES
                out[v * n_data + d, j * CAP : (j + 1) * CAP, :] = rows[
                    v * CAP : (v + 1) * CAP, column : column + LANES
                ]
        strip = pl.ds(v * n_data, n_data)
        stores.append(pltpu.make_async_copy(out.at[strip], out_hbm.at[strip], out_sem.at[v]))
        stores[-1].start()
    for store in stores:
        store.wait()


def pack(rows, n_vocab, n_data):
    shape = (n_vocab * n_data, rows.shape[1] // (n_data * LANES) * CAP, LANES)
    return pl.pallas_call(
        functools.partial(pack_kernel, n_vocab, n_data),
        out_shape=jax.ShapeDtypeStruct(shape, rows.dtype),
        in_specs=[pl.BlockSpec(memory_space=pl.ANY)],
        out_specs=pl.BlockSpec(memory_space=pl.ANY),
        scratch_shapes=[
            pltpu.VMEM(rows.shape, rows.dtype),
            pltpu.VMEM(shape, rows.dtype),
            pltpu.SemaphoreType.DMA((n_vocab,)),
            pltpu.SemaphoreType.DMA((n_vocab,)),
        ],
        name="pack",
    )(rows)


def exchange_ids(ids, n_vocab, n_data):
    def from_device(x, apart):
        return lax.ppermute(x, AXES, [(i, i ^ apart) for i in range(n_vocab * n_data)])

    ids = jnp.concatenate([ids, from_device(ids, 1)])
    ids = jnp.concatenate([ids] + [from_device(ids, v * n_data) for v in range(1, n_vocab)])
    return [ids] + [from_device(ids, z) for z in range(2, n_data, 2)]


def place_kernel(n_vocab, n_data, *refs):
    parts_in = refs[: n_data // 2]
    out, ids_s = refs[n_data // 2 :]
    chunks = ids_s.shape[0]
    total = chunks * LANES
    vocab = lax.axis_index("vocab")
    near = 2 * n_vocab
    lane = lax.broadcasted_iota(jnp.int32, (near, LANES), 1)
    sub = lax.broadcasted_iota(jnp.int32, (near, LANES), 0)
    here = lax.div(lane, CAP) == lax.rem(sub, GROUP)
    for z in range(n_data // 2):
        mine = parts_in[z][:, :CAP]
        for v in range(1, n_vocab):
            mine = jnp.where(vocab == v, parts_in[z][:, v * CAP : (v + 1) * CAP], mine)
        mine = jnp.where(here, jnp.concatenate([mine] * GROUP, axis=1), 0)
        for i in range(near // GROUP):
            row = z * (near // GROUP) + i
            ids_s[row : row + 1, :] = jnp.sum(mine[i * GROUP : (i + 1) * GROUP], axis=0, keepdims=True)
    ids = ids_s[...]
    ids = jnp.where(ids < 0, BLOCKS * BLOCK, ids - vocab * VOCAB_DEV)
    out[:chunks, :] = ids

    block = lax.div(ids, BLOCK)
    inside = [jnp.where(block == b, 1.0, 0.0) for b in range(BLOCKS)]
    mask = jnp.concatenate(inside, axis=0).astype(jnp.bfloat16)
    above = lax.broadcasted_iota(jnp.int32, (LANES, 2 * LANES), 0) < lax.broadcasted_iota(
        jnp.int32, (LANES, 2 * LANES), 1
    )
    ahead = jnp.dot(mask, jnp.where(above, 1.0, 0.0).astype(jnp.bfloat16), preferred_element_type=jnp.float32)
    groups = BLOCKS * chunks
    below = lax.broadcasted_iota(jnp.int32, (groups, groups), 0) > lax.broadcasted_iota(jnp.int32, (groups, groups), 1)
    earlier = jnp.dot(
        jnp.where(below, 1.0, 0.0).astype(jnp.bfloat16), ahead[:, LANES:].astype(jnp.bfloat16), preferred_element_type=jnp.float32
    )
    ahead = ahead[:, :LANES] + earlier
    place = jnp.where(block < BLOCKS, 0.0, float(total))
    for b in range(BLOCKS):
        place = place + inside[b] * ahead[b * chunks : (b + 1) * chunks]
    out[chunks:, :] = place.astype(jnp.int32)


def place_tokens(ids, n_vocab, n_data):
    shape = (n_vocab * n_data * CAP // LANES, LANES)
    return pl.pallas_call(
        functools.partial(place_kernel, n_vocab, n_data),
        out_shape=jax.ShapeDtypeStruct((2 * shape[0], LANES), jnp.int32),
        in_specs=[pl.BlockSpec(memory_space=pltpu.VMEM)] * len(ids),
        out_specs=pl.BlockSpec(memory_space=pltpu.VMEM),
        scratch_shapes=[pltpu.VMEM(shape, jnp.int32)],
        compiler_params=pltpu.CompilerParams(vmem_limit_bytes=4 * 1024 * 1024),
        name="place",
    )(*ids)


def table_kernel(
    scale, n_vocab, n_data, got, placed, table_hbm, share_hbm, x, sorted_ids, sorted_x, table, share, starts, sem
):
    sources, length, _ = got.shape
    total = sources * CAP
    chunks = total // LANES
    tiles = length // CAP
    vocab, data = lax.axis_index("vocab"), lax.axis_index("dp")
    ids = placed[:chunks, :]
    place = placed[chunks:, :]
    for b in range(BLOCKS + 1):
        starts[b] = jnp.sum((ids < b * BLOCK).astype(jnp.int32))
    for z in range(n_data // 2):
        for v in range(n_vocab):
            for c in range(2):
                source = jnp.bitwise_xor(vocab, v) * n_data + jnp.bitwise_xor(data, 2 * z + c)
                at = ((z * n_vocab + v) * 2 + c) * CAP
                for j in range(tiles):
                    x[at : at + CAP, j * LANES : (j + 1) * LANES] = got[source, j * CAP : (j + 1) * CAP, :]
    sorted_ids[...] = jnp.full(sorted_ids.shape, -1, jnp.int32)
    sorted_x[...] = jnp.zeros(sorted_x.shape, x.dtype)

    flat = jnp.concatenate([ids[p : p + 1, :] for p in range(chunks)], axis=1)
    pick = lax.broadcasted_iota(jnp.int32, (8, total), 0)
    parts = jnp.where(pick == 0, lax.shift_right_arithmetic(flat, 7), jnp.bitwise_and(flat, 127))
    parts = parts.astype(jnp.float32).astype(x.dtype)

    def order(c):
        at = lax.broadcasted_iota(jnp.int32, (WINDOW, LANES), 0) + c * WINDOW
        move = jnp.concatenate(
            [jnp.where(place[p : p + 1, :] == at, 1.0, 0.0).astype(x.dtype) for p in range(chunks)], axis=1
        )
        moved = lax.dot_general(parts, move, (((1,), (1,)), ((), ())), preferred_element_type=jnp.float32)
        moved = (moved[0:1] * 128.0 + moved[1:2]).astype(jnp.int32)
        for i in range(WINDOW // LANES):
            row = c * (WINDOW // LANES) + i
            sorted_ids[row : row + 1, :] = moved[:, i * LANES : (i + 1) * LANES]
        sorted_x[c * WINDOW : (c + 1) * WINDOW, :] = jnp.dot(
            move, x[...], preferred_element_type=jnp.float32
        ).astype(x.dtype)

    def rows_of(b, k):
        row = lax.broadcasted_iota(jnp.int32, (BLOCK, LANES), 0) + b * BLOCK
        hit = jnp.concatenate(
            [
                jnp.where(sorted_ids[pl.ds(k + i, 1), :] == row, 1.0, 0.0).astype(x.dtype)
                for i in range(WINDOW // LANES)
            ],
            axis=1,
        )
        at = pl.ds(pl.multiple_of(k * LANES, LANES), WINDOW)
        return jnp.dot(hit, sorted_x[at, :], preferred_element_type=jnp.float32)

    def out_copy(b):
        at = pl.ds(b * BLOCK, min(BLOCK, VOCAB_DEV - b * BLOCK))
        return pltpu.make_async_copy(table.at[at, :], table_hbm.at[at, :], sem.at[b])

    def window_of(b):
        return jnp.minimum(lax.shift_right_logical(starts[b], 7), chunks - 1)

    windows = total // WINDOW
    short = jnp.int32(0)
    built = 0
    for c in range(windows):
        order(c)
        ready = BLOCKS if c == windows - 1 else max((c + 1) * BLOCKS // windows - 2, 0)
        for b in range(built, ready):
            table[b * BLOCK : (b + 1) * BLOCK, :] = rows_of(b, window_of(b))
            out_copy(b).start()
        if ready > built:
            short = jnp.maximum(short, starts[ready] - (c + 1) * WINDOW)
        built = max(built, ready)
    for b in range(BLOCKS):
        short = jnp.maximum(short, starts[b + 1] - window_of(b) * LANES - WINDOW)

    def spread(size, value):
        of = lax.broadcasted_iota(jnp.int32, (size, LANES), 0)
        return jnp.concatenate(
            [jnp.where(value[p : p + 1, :] == of, 1.0, 0.0).astype(x.dtype) for p in range(chunks)], axis=1
        )

    share[...] = scale * lax.dot_general(
        spread(BLOCKS * BLOCK // LANES, lax.shift_right_arithmetic(ids, 7)),
        spread(LANES, jnp.bitwise_and(ids, 127)),
        (((1,), (1,)), ((), ())),
        preferred_element_type=jnp.float32,
    )
    share_copy = pltpu.make_async_copy(share, share_hbm, sem.at[BLOCKS])
    share_copy.start()

    @pl.when(short > 0)
    def _():
        for b in range(BLOCKS):
            out_copy(b).wait()

        def again(b, _):
            at = pl.ds(pl.multiple_of(b * BLOCK, BLOCK), BLOCK)
            table[at, :] = jnp.zeros((BLOCK, table.shape[1]), jnp.float32)

            def window(w, _):
                table[at, :] += rows_of(b, window_of(b) + w * (WINDOW // LANES))
                return 0

            count = lax.div(jnp.maximum(starts[b + 1] - window_of(b) * LANES + WINDOW - 1, 0), WINDOW)
            return lax.fori_loop(0, count, window, 0)

        lax.fori_loop(0, BLOCKS, again, 0)
        for b in range(BLOCKS):
            out_copy(b).start()

    for b in range(BLOCKS):
        out_copy(b).wait()
    share_copy.wait()


def make_table(got, placed, scale, n_vocab, n_data):
    sources, length, _ = got.shape
    total = sources * CAP
    chunks = total // LANES
    width = length // CAP * LANES
    return pl.pallas_call(
        functools.partial(table_kernel, scale, n_vocab, n_data),
        out_shape=(
            jax.ShapeDtypeStruct((VOCAB_DEV, width), jnp.float32),
            jax.ShapeDtypeStruct((BLOCKS * BLOCK // LANES, LANES), jnp.float32),
        ),
        in_specs=[pl.BlockSpec(memory_space=pltpu.VMEM)] * 2,
        out_specs=(pl.BlockSpec(memory_space=pl.ANY), pl.BlockSpec(memory_space=pl.ANY)),
        scratch_shapes=[
            pltpu.VMEM((total, width), got.dtype),
            pltpu.VMEM((chunks + 8, LANES), jnp.int32),
            pltpu.VMEM((total + LANES, width), got.dtype),
            pltpu.VMEM((BLOCKS * BLOCK, width), jnp.float32),
            pltpu.VMEM((BLOCKS * BLOCK // LANES, LANES), jnp.float32),
            pltpu.SMEM((BLOCKS + 1,), jnp.int32),
            pltpu.SemaphoreType.DMA((BLOCKS + 1,)),
        ],
        compiler_params=pltpu.CompilerParams(vmem_limit_bytes=48 * 1024 * 1024),
        name="table",
    )(got, placed)


def local(grads, token_ids):
    n_vocab = lax.axis_size("vocab")
    n_data = lax.axis_size("dp")
    rows, ids = bucket(token_ids, grads, n_vocab)
    got = lax.all_to_all(pack(rows, n_vocab, n_data), AXES, split_axis=0, concat_axis=0, tiled=True)
    placed = place_tokens(exchange_ids(ids, n_vocab, n_data), n_vocab, n_data)
    table, share = make_table(got, placed, VOCAB_DEV / (TOK_DEV * n_data), n_vocab, n_data)
    return table, share.reshape(-1)[:VOCAB_DEV]


def solution(mesh):
    in_specs = (P(AXES, None), P(AXES))
    out_specs = (P("vocab", "dp"), P("vocab"))
    return jax.shard_map(local, mesh=mesh, in_specs=in_specs, out_specs=out_specs, check_vma=False)
```

```python
import functools

import jax
import jax.numpy as jnp
from jax import lax
from jax.experimental import pallas as pl
from jax.experimental.pallas import tpu as pltpu
from jax.sharding import PartitionSpec as P


VOCAB_DEV = 8016
TOK_DEV = 128
CAP = 32
AXES = ("vocab", "dp")
LANES = 128
GROUP = LANES // CAP
BLOCK = 512
BLOCKS = -(-VOCAB_DEV // BLOCK)
WINDOW = 256


def bucket(ids, data, n_vocab):
    length = ids.shape[0]
    if n_vocab * CAP == length:
        return data, ids.reshape(1, length)
    owner_start = jnp.arange(n_vocab, dtype=jnp.int32) * VOCAB_DEV
    starts = jnp.sum((ids[None, :] < owner_start[:, None]).astype(jnp.int32), axis=1)
    finish = jnp.concatenate([starts[1:], jnp.full((1,), length, jnp.int32)])
    slot = jnp.arange(CAP, dtype=jnp.int32)
    places = starts[:, None] + slot[None, :]
    valid = places < finish[:, None]
    columns = jnp.arange(length, dtype=jnp.int32)
    select = (places[:, :, None] == columns) & valid[:, :, None]
    rows = jnp.einsum(
        "vcl,ld->vcd", select.astype(data.dtype), data, preferred_element_type=jnp.float32
    ).astype(data.dtype)
    picked = jnp.sum(jnp.where(select, ids, 0), axis=2)
    slot_ids = jnp.where(valid, picked, -1)
    return rows.reshape(n_vocab * CAP, data.shape[1]), slot_ids.reshape(1, n_vocab * CAP)


def pack_kernel(n_vocab, n_data, rows_hbm, out_hbm, rows, out, in_sem, out_sem):
    tiles = rows.shape[1] // (n_data * LANES)
    loads = []
    for v in range(n_vocab):
        strip = pl.ds(v * CAP, CAP)
        loads.append(pltpu.make_async_copy(rows_hbm.at[strip], rows.at[strip], in_sem.at[v]))
        loads[-1].start()
    stores = []
    for v in range(n_vocab):
        loads[v].wait()
        for d in range(n_data):
            for j in range(tiles):
                column = (d * tiles + j) * LANES
                out[v * n_data + d, j * CAP : (j + 1) * CAP, :] = rows[
                    v * CAP : (v + 1) * CAP, column : column + LANES
                ]
        strip = pl.ds(v * n_data, n_data)
        stores.append(pltpu.make_async_copy(out.at[strip], out_hbm.at[strip], out_sem.at[v]))
        stores[-1].start()
    for store in stores:
        store.wait()


def pack(rows, n_vocab, n_data):
    shape = (n_vocab * n_data, rows.shape[1] // (n_data * LANES) * CAP, LANES)
    return pl.pallas_call(
        functools.partial(pack_kernel, n_vocab, n_data),
        out_shape=jax.ShapeDtypeStruct(shape, rows.dtype),
        in_specs=[pl.BlockSpec(memory_space=pl.ANY)],
        out_specs=pl.BlockSpec(memory_space=pl.ANY),
        scratch_shapes=[
            pltpu.VMEM(rows.shape, rows.dtype),
            pltpu.VMEM(shape, rows.dtype),
            pltpu.SemaphoreType.DMA((n_vocab,)),
            pltpu.SemaphoreType.DMA((n_vocab,)),
        ],
        name="pack",
    )(rows)


def exchange_ids(ids, n_vocab, n_data):
    def from_device(x, apart):
        return lax.ppermute(x, AXES, [(i, i ^ apart) for i in range(n_vocab * n_data)])

    ids = jnp.concatenate([ids, from_device(ids, 1)])
    ids = jnp.concatenate([ids] + [from_device(ids, v * n_data) for v in range(1, n_vocab)])
    return [ids] + [from_device(ids, z) for z in range(2, n_data, 2)]


def moves(place, c, dtype):
    at = lax.broadcasted_iota(jnp.int32, (WINDOW, LANES), 0) + c * WINDOW
    return jnp.concatenate(
        [jnp.where(place[p : p + 1, :] == at, 1.0, 0.0).astype(dtype) for p in range(place.shape[0])], axis=1
    )


def place_kernel(n_vocab, n_data, *refs):
    parts_in = refs[: n_data // 2]
    out, first, ids_s = refs[n_data // 2 :]
    chunks = ids_s.shape[0]
    total = chunks * LANES
    vocab = lax.axis_index("vocab")
    near = 2 * n_vocab
    lane = lax.broadcasted_iota(jnp.int32, (near, LANES), 1)
    sub = lax.broadcasted_iota(jnp.int32, (near, LANES), 0)
    here = lax.div(lane, CAP) == lax.rem(sub, GROUP)
    for z in range(n_data // 2):
        mine = parts_in[z][:, :CAP]
        for v in range(1, n_vocab):
            mine = jnp.where(vocab == v, parts_in[z][:, v * CAP : (v + 1) * CAP], mine)
        mine = jnp.where(here, jnp.concatenate([mine] * GROUP, axis=1), 0)
        for i in range(near // GROUP):
            row = z * (near // GROUP) + i
            ids_s[row : row + 1, :] = jnp.sum(mine[i * GROUP : (i + 1) * GROUP], axis=0, keepdims=True)
    ids = ids_s[...]
    ids = jnp.where(ids < 0, BLOCKS * BLOCK, ids - vocab * VOCAB_DEV)
    out[:chunks, :] = ids

    block = lax.div(ids, BLOCK)
    inside = [jnp.where(block == b, 1.0, 0.0) for b in range(BLOCKS)]
    mask = jnp.concatenate(inside, axis=0).astype(jnp.bfloat16)
    above = lax.broadcasted_iota(jnp.int32, (LANES, 2 * LANES), 0) < lax.broadcasted_iota(
        jnp.int32, (LANES, 2 * LANES), 1
    )
    ahead = jnp.dot(mask, jnp.where(above, 1.0, 0.0).astype(jnp.bfloat16), preferred_element_type=jnp.float32)
    groups = BLOCKS * chunks
    below = lax.broadcasted_iota(jnp.int32, (groups, groups), 0) > lax.broadcasted_iota(jnp.int32, (groups, groups), 1)
    earlier = jnp.dot(
        jnp.where(below, 1.0, 0.0).astype(jnp.bfloat16), ahead[:, LANES:].astype(jnp.bfloat16), preferred_element_type=jnp.float32
    )
    ahead = ahead[:, :LANES] + earlier
    place = jnp.where(block < BLOCKS, 0.0, float(total))
    for b in range(BLOCKS):
        place = place + inside[b] * ahead[b * chunks : (b + 1) * chunks]
    place = place.astype(jnp.int32)
    out[chunks:, :] = place
    first[...] = moves(place, 0, first.dtype)


def place_tokens(ids, n_vocab, n_data):
    shape = (n_vocab * n_data * CAP // LANES, LANES)
    return pl.pallas_call(
        functools.partial(place_kernel, n_vocab, n_data),
        out_shape=(
            jax.ShapeDtypeStruct((2 * shape[0], LANES), jnp.int32),
            jax.ShapeDtypeStruct((WINDOW, shape[0] * LANES), jnp.bfloat16),
        ),
        in_specs=[pl.BlockSpec(memory_space=pltpu.VMEM)] * len(ids),
        out_specs=(pl.BlockSpec(memory_space=pltpu.VMEM),) * 2,
        scratch_shapes=[pltpu.VMEM(shape, jnp.int32)],
        compiler_params=pltpu.CompilerParams(vmem_limit_bytes=4 * 1024 * 1024),
        name="place",
    )(*ids)


def table_kernel(
    scale, n_vocab, n_data, got, placed, first, table_hbm, share_hbm, x, sorted_ids, sorted_x, table, share, starts, sem
):
    sources, length, _ = got.shape
    total = sources * CAP
    chunks = total // LANES
    tiles = length // CAP
    vocab, data = lax.axis_index("vocab"), lax.axis_index("dp")
    ids = placed[:chunks, :]
    place = placed[chunks:, :]
    for b in range(BLOCKS + 1):
        starts[b] = jnp.sum((ids < b * BLOCK).astype(jnp.int32))
    for z in range(n_data // 2):
        for v in range(n_vocab):
            for c in range(2):
                source = jnp.bitwise_xor(vocab, v) * n_data + jnp.bitwise_xor(data, 2 * z + c)
                at = ((z * n_vocab + v) * 2 + c) * CAP
                for j in range(tiles):
                    x[at : at + CAP, j * LANES : (j + 1) * LANES] = got[source, j * CAP : (j + 1) * CAP, :]
    sorted_ids[...] = jnp.full(sorted_ids.shape, -1, jnp.int32)
    sorted_x[...] = jnp.zeros(sorted_x.shape, x.dtype)

    flat = jnp.concatenate([ids[p : p + 1, :] for p in range(chunks)], axis=1)
    pick = lax.broadcasted_iota(jnp.int32, (8, total), 0)
    parts = jnp.where(pick == 0, lax.shift_right_arithmetic(flat, 7), jnp.bitwise_and(flat, 127))
    parts = parts.astype(jnp.float32).astype(x.dtype)

    def order(c):
        move = first[...] if c == 0 else moves(place, c, x.dtype)
        moved = lax.dot_general(parts, move, (((1,), (1,)), ((), ())), preferred_element_type=jnp.float32)
        moved = (moved[0:1] * 128.0 + moved[1:2]).astype(jnp.int32)
        for i in range(WINDOW // LANES):
            row = c * (WINDOW // LANES) + i
            sorted_ids[row : row + 1, :] = moved[:, i * LANES : (i + 1) * LANES]
        sorted_x[c * WINDOW : (c + 1) * WINDOW, :] = jnp.dot(
            move, x[...], preferred_element_type=jnp.float32
        ).astype(x.dtype)

    def rows_of(b, k):
        row = lax.broadcasted_iota(jnp.int32, (BLOCK, LANES), 0) + b * BLOCK
        hit = jnp.concatenate(
            [
                jnp.where(sorted_ids[pl.ds(k + i, 1), :] == row, 1.0, 0.0).astype(x.dtype)
                for i in range(WINDOW // LANES)
            ],
            axis=1,
        )
        at = pl.ds(pl.multiple_of(k * LANES, LANES), WINDOW)
        return jnp.dot(hit, sorted_x[at, :], preferred_element_type=jnp.float32)

    def out_copy(b):
        at = pl.ds(b * BLOCK, min(BLOCK, VOCAB_DEV - b * BLOCK))
        return pltpu.make_async_copy(table.at[at, :], table_hbm.at[at, :], sem.at[b])

    def window_of(b):
        return jnp.minimum(lax.shift_right_logical(starts[b], 7), chunks - 1)

    windows = total // WINDOW
    short = jnp.int32(0)
    built = 0
    for c in range(windows):
        order(c)
        ready = BLOCKS if c == windows - 1 else max((c + 1) * BLOCKS // windows - 2, 0)
        for b in range(built, ready):
            table[b * BLOCK : (b + 1) * BLOCK, :] = rows_of(b, window_of(b))
            out_copy(b).start()
        if ready > built:
            short = jnp.maximum(short, starts[ready] - (c + 1) * WINDOW)
        built = max(built, ready)
    for b in range(BLOCKS):
        short = jnp.maximum(short, starts[b + 1] - window_of(b) * LANES - WINDOW)

    def spread(size, value):
        of = lax.broadcasted_iota(jnp.int32, (size, LANES), 0)
        return jnp.concatenate(
            [jnp.where(value[p : p + 1, :] == of, 1.0, 0.0).astype(x.dtype) for p in range(chunks)], axis=1
        )

    share[...] = scale * lax.dot_general(
        spread(BLOCKS * BLOCK // LANES, lax.shift_right_arithmetic(ids, 7)),
        spread(LANES, jnp.bitwise_and(ids, 127)),
        (((1,), (1,)), ((), ())),
        preferred_element_type=jnp.float32,
    )
    share_copy = pltpu.make_async_copy(share, share_hbm, sem.at[BLOCKS])
    share_copy.start()

    @pl.when(short > 0)
    def _():
        for b in range(BLOCKS):
            out_copy(b).wait()

        def again(b, _):
            at = pl.ds(pl.multiple_of(b * BLOCK, BLOCK), BLOCK)
            table[at, :] = jnp.zeros((BLOCK, table.shape[1]), jnp.float32)

            def window(w, _):
                table[at, :] += rows_of(b, window_of(b) + w * (WINDOW // LANES))
                return 0

            count = lax.div(jnp.maximum(starts[b + 1] - window_of(b) * LANES + WINDOW - 1, 0), WINDOW)
            return lax.fori_loop(0, count, window, 0)

        lax.fori_loop(0, BLOCKS, again, 0)
        for b in range(BLOCKS):
            out_copy(b).start()

    for b in range(BLOCKS):
        out_copy(b).wait()
    share_copy.wait()


def make_table(got, placed, first, scale, n_vocab, n_data):
    sources, length, _ = got.shape
    total = sources * CAP
    chunks = total // LANES
    width = length // CAP * LANES
    return pl.pallas_call(
        functools.partial(table_kernel, scale, n_vocab, n_data),
        out_shape=(
            jax.ShapeDtypeStruct((VOCAB_DEV, width), jnp.float32),
            jax.ShapeDtypeStruct((BLOCKS * BLOCK // LANES, LANES), jnp.float32),
        ),
        in_specs=[pl.BlockSpec(memory_space=pltpu.VMEM)] * 3,
        out_specs=(pl.BlockSpec(memory_space=pl.ANY), pl.BlockSpec(memory_space=pl.ANY)),
        scratch_shapes=[
            pltpu.VMEM((total, width), got.dtype),
            pltpu.VMEM((chunks + 8, LANES), jnp.int32),
            pltpu.VMEM((total + LANES, width), got.dtype),
            pltpu.VMEM((BLOCKS * BLOCK, width), jnp.float32),
            pltpu.VMEM((BLOCKS * BLOCK // LANES, LANES), jnp.float32),
            pltpu.SMEM((BLOCKS + 1,), jnp.int32),
            pltpu.SemaphoreType.DMA((BLOCKS + 1,)),
        ],
        compiler_params=pltpu.CompilerParams(vmem_limit_bytes=48 * 1024 * 1024),
        name="table",
    )(got, placed, first)


def local(grads, token_ids):
    n_vocab = lax.axis_size("vocab")
    n_data = lax.axis_size("dp")
    rows, ids = bucket(token_ids, grads, n_vocab)
    got = lax.all_to_all(pack(rows, n_vocab, n_data), AXES, split_axis=0, concat_axis=0, tiled=True)
    placed, first = place_tokens(exchange_ids(ids, n_vocab, n_data), n_vocab, n_data)
    table, share = make_table(got, placed, first, VOCAB_DEV / (TOK_DEV * n_data), n_vocab, n_data)
    return table, share.reshape(-1)[:VOCAB_DEV]


def solution(mesh):
    in_specs = (P(AXES, None), P(AXES))
    out_specs = (P("vocab", "dp"), P("vocab"))
    return jax.shard_map(local, mesh=mesh, in_specs=in_specs, out_specs=out_specs, check_vma=False)
```

```python
import functools

import jax
import jax.numpy as jnp
from jax import lax
from jax.experimental import pallas as pl
from jax.experimental.pallas import tpu as pltpu
from jax.sharding import PartitionSpec as P


VOCAB_DEV = 8016
TOK_DEV = 128
CAP = 32
AXES = ("vocab", "dp")
LANES = 128
GROUP = LANES // CAP
BLOCK = 512
BLOCKS = -(-VOCAB_DEV // BLOCK)
WINDOW = 256


def bucket(ids, data, n_vocab):
    length = ids.shape[0]
    if n_vocab * CAP == length:
        return data, ids.reshape(1, length)
    owner_start = jnp.arange(n_vocab, dtype=jnp.int32) * VOCAB_DEV
    starts = jnp.sum((ids[None, :] < owner_start[:, None]).astype(jnp.int32), axis=1)
    finish = jnp.concatenate([starts[1:], jnp.full((1,), length, jnp.int32)])
    slot = jnp.arange(CAP, dtype=jnp.int32)
    places = starts[:, None] + slot[None, :]
    valid = places < finish[:, None]
    columns = jnp.arange(length, dtype=jnp.int32)
    select = (places[:, :, None] == columns) & valid[:, :, None]
    rows = jnp.einsum(
        "vcl,ld->vcd", select.astype(data.dtype), data, preferred_element_type=jnp.float32
    ).astype(data.dtype)
    picked = jnp.sum(jnp.where(select, ids, 0), axis=2)
    slot_ids = jnp.where(valid, picked, -1)
    return rows.reshape(n_vocab * CAP, data.shape[1]), slot_ids.reshape(1, n_vocab * CAP)


def pack_kernel(n_vocab, n_data, rows_hbm, out_hbm, rows, out, in_sem, out_sem):
    tiles = rows.shape[1] // (n_data * LANES)
    loads = []
    for v in range(n_vocab):
        strip = pl.ds(v * CAP, CAP)
        loads.append(pltpu.make_async_copy(rows_hbm.at[strip], rows.at[strip], in_sem.at[v]))
        loads[-1].start()
    stores = []
    for v in range(n_vocab):
        loads[v].wait()
        for d in range(n_data):
            for j in range(tiles):
                column = (d * tiles + j) * LANES
                out[v * n_data + d, j * CAP : (j + 1) * CAP, :] = rows[
                    v * CAP : (v + 1) * CAP, column : column + LANES
                ]
        strip = pl.ds(v * n_data, n_data)
        stores.append(pltpu.make_async_copy(out.at[strip], out_hbm.at[strip], out_sem.at[v]))
        stores[-1].start()
    for store in stores:
        store.wait()


def pack(rows, n_vocab, n_data):
    shape = (n_vocab * n_data, rows.shape[1] // (n_data * LANES) * CAP, LANES)
    return pl.pallas_call(
        functools.partial(pack_kernel, n_vocab, n_data),
        out_shape=jax.ShapeDtypeStruct(shape, rows.dtype),
        in_specs=[pl.BlockSpec(memory_space=pl.ANY)],
        out_specs=pl.BlockSpec(memory_space=pl.ANY),
        scratch_shapes=[
            pltpu.VMEM(rows.shape, rows.dtype),
            pltpu.VMEM(shape, rows.dtype),
            pltpu.SemaphoreType.DMA((n_vocab,)),
            pltpu.SemaphoreType.DMA((n_vocab,)),
        ],
        name="pack",
    )(rows)


def exchange_ids(ids, n_vocab, n_data):
    def from_device(x, apart):
        return lax.ppermute(x, AXES, [(i, i ^ apart) for i in range(n_vocab * n_data)])

    ids = jnp.concatenate([ids, from_device(ids, 1)])
    ids = jnp.concatenate([ids] + [from_device(ids, v * n_data) for v in range(1, n_vocab)])
    return [ids] + [from_device(ids, z) for z in range(2, n_data, 2)]


def place_kernel(n_vocab, n_data, *refs):
    parts_in = refs[: n_data // 2]
    out, ids_s = refs[n_data // 2 :]
    chunks = ids_s.shape[0]
    total = chunks * LANES
    vocab = lax.axis_index("vocab")
    near = 2 * n_vocab
    lane = lax.broadcasted_iota(jnp.int32, (near, LANES), 1)
    sub = lax.broadcasted_iota(jnp.int32, (near, LANES), 0)
    here = lax.div(lane, CAP) == lax.rem(sub, GROUP)
    for z in range(n_data // 2):
        mine = parts_in[z][:, :CAP]
        for v in range(1, n_vocab):
            mine = jnp.where(vocab == v, parts_in[z][:, v * CAP : (v + 1) * CAP], mine)
        mine = jnp.where(here, jnp.concatenate([mine] * GROUP, axis=1), 0)
        for i in range(near // GROUP):
            row = z * (near // GROUP) + i
            ids_s[row : row + 1, :] = jnp.sum(mine[i * GROUP : (i + 1) * GROUP], axis=0, keepdims=True)
    ids = ids_s[...]
    ids = jnp.where(ids < 0, BLOCKS * BLOCK, ids - vocab * VOCAB_DEV)
    out[:chunks, :] = ids

    block = lax.div(ids, BLOCK)
    inside = [jnp.where(block == b, 1.0, 0.0) for b in range(BLOCKS)]
    mask = jnp.concatenate(inside, axis=0).astype(jnp.bfloat16)
    above = lax.broadcasted_iota(jnp.int32, (LANES, 2 * LANES), 0) < lax.broadcasted_iota(
        jnp.int32, (LANES, 2 * LANES), 1
    )
    ahead = jnp.dot(mask, jnp.where(above, 1.0, 0.0).astype(jnp.bfloat16), preferred_element_type=jnp.float32)
    groups = BLOCKS * chunks
    below = lax.broadcasted_iota(jnp.int32, (groups, groups), 0) > lax.broadcasted_iota(jnp.int32, (groups, groups), 1)
    earlier = jnp.dot(
        jnp.where(below, 1.0, 0.0).astype(jnp.bfloat16), ahead[:, LANES:].astype(jnp.bfloat16), preferred_element_type=jnp.float32
    )
    ahead = ahead[:, :LANES] + earlier
    place = jnp.where(block < BLOCKS, 0.0, float(total))
    for b in range(BLOCKS):
        place = place + inside[b] * ahead[b * chunks : (b + 1) * chunks]
    out[chunks:, :] = place.astype(jnp.int32)


def place_tokens(ids, n_vocab, n_data):
    shape = (n_vocab * n_data * CAP // LANES, LANES)
    return pl.pallas_call(
        functools.partial(place_kernel, n_vocab, n_data),
        out_shape=jax.ShapeDtypeStruct((2 * shape[0], LANES), jnp.int32),
        in_specs=[pl.BlockSpec(memory_space=pltpu.VMEM)] * len(ids),
        out_specs=pl.BlockSpec(memory_space=pltpu.VMEM),
        scratch_shapes=[pltpu.VMEM(shape, jnp.int32)],
        compiler_params=pltpu.CompilerParams(vmem_limit_bytes=4 * 1024 * 1024),
        name="place",
    )(*ids)


def table_kernel(
    scale, n_vocab, n_data, got, placed, table_hbm, share_hbm, x, sorted_ids, sorted_x, table, share, starts, sem
):
    sources, length, _ = got.shape
    total = sources * CAP
    chunks = total // LANES
    tiles = length // CAP
    vocab, data = lax.axis_index("vocab"), lax.axis_index("dp")
    ids = placed[:chunks, :]
    place = placed[chunks:, :]
    for b in range(BLOCKS + 1):
        starts[b] = jnp.sum((ids < b * BLOCK).astype(jnp.int32))
    for z in range(n_data // 2):
        for v in range(n_vocab):
            for c in range(2):
                source = jnp.bitwise_xor(vocab, v) * n_data + jnp.bitwise_xor(data, 2 * z + c)
                at = ((z * n_vocab + v) * 2 + c) * CAP
                for j in range(tiles):
                    x[at : at + CAP, j * LANES : (j + 1) * LANES] = got[source, j * CAP : (j + 1) * CAP, :]
    sorted_ids[...] = jnp.full(sorted_ids.shape, -1, jnp.int32)
    sorted_x[...] = jnp.zeros(sorted_x.shape, x.dtype)

    flat = jnp.concatenate([ids[p : p + 1, :] for p in range(chunks)], axis=1)
    pick = lax.broadcasted_iota(jnp.int32, (8, total), 0)
    parts = jnp.where(pick == 0, lax.shift_right_arithmetic(flat, 7), jnp.bitwise_and(flat, 127))
    parts = parts.astype(jnp.float32).astype(x.dtype)

    def order(start, size):
        at = lax.broadcasted_iota(jnp.int32, (size, LANES), 0) + start
        move = jnp.concatenate(
            [jnp.where(place[p : p + 1, :] == at, 1.0, 0.0).astype(x.dtype) for p in range(chunks)], axis=1
        )
        moved = lax.dot_general(parts, move, (((1,), (1,)), ((), ())), preferred_element_type=jnp.float32)
        moved = (moved[0:1] * 128.0 + moved[1:2]).astype(jnp.int32)
        for i in range(size // LANES):
            row = start // LANES + i
            sorted_ids[row : row + 1, :] = moved[:, i * LANES : (i + 1) * LANES]
        sorted_x[start : start + size, :] = jnp.dot(
            move, x[...], preferred_element_type=jnp.float32
        ).astype(x.dtype)

    def rows_of(b, k):
        row = lax.broadcasted_iota(jnp.int32, (BLOCK, LANES), 0) + b * BLOCK
        hit = jnp.concatenate(
            [
                jnp.where(sorted_ids[pl.ds(k + i, 1), :] == row, 1.0, 0.0).astype(x.dtype)
                for i in range(WINDOW // LANES)
            ],
            axis=1,
        )
        at = pl.ds(k * LANES if isinstance(k, int) else pl.multiple_of(k * LANES, LANES), WINDOW)
        return jnp.dot(hit, sorted_x[at, :], preferred_element_type=jnp.float32)

    def out_copy(b):
        at = pl.ds(b * BLOCK, min(BLOCK, VOCAB_DEV - b * BLOCK))
        return pltpu.make_async_copy(table.at[at, :], table_hbm.at[at, :], sem.at[b])

    def window_of(b):
        if isinstance(b, int) and b == 0:
            return 0
        return jnp.minimum(lax.shift_right_logical(starts[b], 7), chunks - 1)

    short = jnp.int32(0)
    built = done = 0
    while done < total:
        size = LANES
        order(done, size)
        done += size
        ready = BLOCKS if done == total else max(done * BLOCKS // total - min(done // LANES, 2), 0)
        for b in range(built, ready):
            table[b * BLOCK : (b + 1) * BLOCK, :] = rows_of(b, window_of(b))
            out_copy(b).start()
        if ready > built:
            short = jnp.maximum(short, starts[ready] - done)
        built = max(built, ready)
    for b in range(BLOCKS):
        short = jnp.maximum(short, starts[b + 1] - window_of(b) * LANES - WINDOW)

    def spread(size, value):
        of = lax.broadcasted_iota(jnp.int32, (size, LANES), 0)
        return jnp.concatenate(
            [jnp.where(value[p : p + 1, :] == of, 1.0, 0.0).astype(x.dtype) for p in range(chunks)], axis=1
        )

    share[...] = scale * lax.dot_general(
        spread(BLOCKS * BLOCK // LANES, lax.shift_right_arithmetic(ids, 7)),
        spread(LANES, jnp.bitwise_and(ids, 127)),
        (((1,), (1,)), ((), ())),
        preferred_element_type=jnp.float32,
    )
    share_copy = pltpu.make_async_copy(share, share_hbm, sem.at[BLOCKS])
    share_copy.start()

    @pl.when(short > 0)
    def _():
        for b in range(BLOCKS):
            out_copy(b).wait()

        def again(b, _):
            at = pl.ds(pl.multiple_of(b * BLOCK, BLOCK), BLOCK)
            table[at, :] = jnp.zeros((BLOCK, table.shape[1]), jnp.float32)

            def window(w, _):
                table[at, :] += rows_of(b, window_of(b) + w * (WINDOW // LANES))
                return 0

            count = lax.div(jnp.maximum(starts[b + 1] - window_of(b) * LANES + WINDOW - 1, 0), WINDOW)
            return lax.fori_loop(0, count, window, 0)

        lax.fori_loop(0, BLOCKS, again, 0)
        for b in range(BLOCKS):
            out_copy(b).start()

    for b in range(BLOCKS):
        out_copy(b).wait()
    share_copy.wait()


def make_table(got, placed, scale, n_vocab, n_data):
    sources, length, _ = got.shape
    total = sources * CAP
    chunks = total // LANES
    width = length // CAP * LANES
    return pl.pallas_call(
        functools.partial(table_kernel, scale, n_vocab, n_data),
        out_shape=(
            jax.ShapeDtypeStruct((VOCAB_DEV, width), jnp.float32),
            jax.ShapeDtypeStruct((BLOCKS * BLOCK // LANES, LANES), jnp.float32),
        ),
        in_specs=[pl.BlockSpec(memory_space=pltpu.VMEM)] * 2,
        out_specs=(pl.BlockSpec(memory_space=pl.ANY), pl.BlockSpec(memory_space=pl.ANY)),
        scratch_shapes=[
            pltpu.VMEM((total, width), got.dtype),
            pltpu.VMEM((chunks + 8, LANES), jnp.int32),
            pltpu.VMEM((total + LANES, width), got.dtype),
            pltpu.VMEM((BLOCKS * BLOCK, width), jnp.float32),
            pltpu.VMEM((BLOCKS * BLOCK // LANES, LANES), jnp.float32),
            pltpu.SMEM((BLOCKS + 1,), jnp.int32),
            pltpu.SemaphoreType.DMA((BLOCKS + 1,)),
        ],
        compiler_params=pltpu.CompilerParams(vmem_limit_bytes=48 * 1024 * 1024),
        name="table",
    )(got, placed)


def local(grads, token_ids):
    n_vocab = lax.axis_size("vocab")
    n_data = lax.axis_size("dp")
    rows, ids = bucket(token_ids, grads, n_vocab)
    got = lax.all_to_all(pack(rows, n_vocab, n_data), AXES, split_axis=0, concat_axis=0, tiled=True)
    placed = place_tokens(exchange_ids(ids, n_vocab, n_data), n_vocab, n_data)
    table, share = make_table(got, placed, VOCAB_DEV / (TOK_DEV * n_data), n_vocab, n_data)
    return table, share.reshape(-1)[:VOCAB_DEV]


def solution(mesh):
    in_specs = (P(AXES, None), P(AXES))
    out_specs = (P("vocab", "dp"), P("vocab"))
    return jax.shard_map(local, mesh=mesh, in_specs=in_specs, out_specs=out_specs, check_vma=False)
```
